32 devices in a mesh: energy: 2 (over y), slab: 4 (over z), orb: 2 (over x), rhs: 2 (over core).
Axes of the slice: x: 2, y: 2, z: 4, core: 2. Of those that a mesh axis runs over, the one named last changes fastest.
Arguments:
- diag_blocks: float32 [16, 192, 384], P(('energy', 'slab'), 'orb'), parts along dimension 0, may hold values from -8 to 8, as said below
- couplings: float32 [16, 192, 384], P(('energy', 'slab')), parts along dimension 0, may hold values from -8 to 8
- sources: float32 [16, 32, 384], P(('energy', 'slab'), ('orb', 'rhs')), parts along dimension 0, may hold values from -8 to 8
Outputs:
- solution: float32 [16, 32, 384], P(('energy', 'slab'), ('orb', 'rhs')), parts along dimension 0
The draws below stay inside these ranges and needn't reach their ends.
There are 2 independent parts, one for each index of `energy`. The reference program is written for one: setup_inputs(seed, part) draws one part's arguments, and reference() takes and returns one part's arrays. A program takes and returns all parts, laid end to end along the dimension named above; each array names one. Nothing has to cross between parts.
Inputs may be any that keep to these rules, and one draw needn't show every extreme that they name: Every diag_blocks[n] is Hermitian, and together with couplings it makes K positive definite with smallest eigenvalue 0.01 or more.
All inputs are finite; a program needn't handle non-finite values.
Results may differ from the reference program's by a relative error of at most 0.0003.
Values sent between devices are 32-bit elements; how exact they have to be, the bound alone decides.
A program may use at most 128 MiB of HBM per device.

```python
import math
import jax
import jax.numpy as jnp
from jax import lax

NO = 192
NL = 8
NRHS = 32


def layer_matrices(key):
    base = jax.random.fold_in(key, 1723)
    keys = jax.random.split(base, 6)
    spread = 0.5 / math.sqrt(2.0 * NO)
    identity = jnp.eye(NO, dtype=jnp.float32)
    left_real = identity + spread * jax.random.normal(keys[0], (NL, NO, NO), jnp.float32)
    left_imag = spread * jax.random.normal(keys[1], (NL, NO, NO), jnp.float32)
    right_real = identity + spread * jax.random.normal(keys[2], (NL, NO, NO), jnp.float32)
    right_imag = spread * jax.random.normal(keys[3], (NL, NO, NO), jnp.float32)
    level_shift = jnp.exp(jax.random.uniform(keys[4], (), jnp.float32, math.log(0.01), math.log(0.03)))
    shifts = level_shift * jnp.exp(jax.random.uniform(keys[5], (NL,), jnp.float32, 0.0, math.log(4.0)))
    return (left_real, left_imag, right_real, right_imag, shifts)


def hermitian_product(first_real, first_imag, second_real, second_imag):
    real_part = jnp.einsum('nki,nkj->nij', first_real, second_real) + jnp.einsum('nki,nkj->nij', first_imag, second_imag)
    imag_part = jnp.einsum('nki,nkj->nij', first_real, second_imag) - jnp.einsum('nki,nkj->nij', first_imag, second_real)
    return (real_part, imag_part)


def column_major(real_part, imag_part):
    return jnp.concatenate([jnp.swapaxes(real_part, 1, 2), jnp.swapaxes(imag_part, 1, 2)], axis=2)


def draw_diag_blocks(key, part):
    left_real, left_imag, right_real, right_imag, shifts = layer_matrices(key)
    own_real, own_imag = hermitian_product(right_real, right_imag, right_real, right_imag)
    next_real, next_imag = hermitian_product(left_real, left_imag, left_real, left_imag)
    has_above = (jnp.arange(NL) >= 1).astype(jnp.float32)[:, None, None]
    padding = jnp.zeros((1, NO, NO), jnp.float32)
    below_real = jnp.concatenate([next_real[1:], padding], axis=0)
    below_imag = jnp.concatenate([next_imag[1:], padding], axis=0)
    identity = jnp.eye(NO, dtype=jnp.float32)
    real_part = has_above * own_real + below_real + shifts[:, None, None] * identity
    imag_part = has_above * own_imag + below_imag
    return column_major(real_part, imag_part)


def draw_couplings(key, part):
    left_real, left_imag, right_real, right_imag, shifts = layer_matrices(key)
    cross_real, cross_imag = hermitian_product(right_real, right_imag, left_real, left_imag)
    has_above = (jnp.arange(NL) >= 1).astype(jnp.float32)[:, None, None]
    return column_major(-has_above * cross_real, -has_above * cross_imag)


def draw_sources(key, part):
    base = jax.random.fold_in(key, 3301)
    keys = jax.random.split(base, 1)
    return jnp.clip(jax.random.normal(keys[0], (NL, NRHS, 2 * NO), jnp.float32), -6.0, 6.0)


def setup_inputs(seed: int = 0, part: int = 0) -> dict:
    seeds = jax.random.split(jax.random.key(seed), 4)
    own_keys = jax.random.split(jax.random.fold_in(seeds[3], part), 4)
    return {
        "diag_blocks": draw_diag_blocks(jax.random.fold_in(jax.random.fold_in(seeds[3], part), 71), part),
        "couplings": draw_couplings(jax.random.fold_in(jax.random.fold_in(seeds[3], part), 71), part),
        "sources": draw_sources(jax.random.fold_in(jax.random.fold_in(seeds[3], part), 71), part),
    }


def embed(columns):
    block_order = columns.shape[-1] // 2
    turned = jnp.concatenate([-columns[..., block_order:], columns[..., :block_order]], axis=-1)
    return jnp.concatenate([columns, turned], axis=-2)

def times(left, right):
    return jnp.dot(left.astype(jnp.float32), right.astype(jnp.float32), precision=lax.Precision.HIGHEST, preferred_element_type=jnp.float32)

def times_flipped(left, right):
    return lax.dot_general(left.astype(jnp.float32), right.astype(jnp.float32), (((1,), (1,)), ((), ())), precision=lax.Precision.HIGHEST, preferred_element_type=jnp.float32)

def apply_inverse(factor, rows):
    return jax.scipy.linalg.cho_solve((factor, True), rows.T).T

def reference(diag_blocks, couplings, sources):
    layer_count = diag_blocks.shape[0]
    block_order = diag_blocks.shape[2] // 2
    keep = (jnp.arange(layer_count) > 0).astype(couplings.dtype)
    couplings = couplings * keep[:, None, None]
    embedded = jax.vmap(embed)(couplings)

    def forward(carry, item):
        factor_prev, load_prev = carry
        block, coupling_embed, source = item
        herm_block = coupling_embed[:, :block_order].T
        pivot = block - times(apply_inverse(factor_prev, herm_block), coupling_embed)
        load = source - times(apply_inverse(factor_prev, load_prev), coupling_embed)
        factor = jnp.linalg.cholesky(embed(pivot))
        return ((factor, load), (factor, load))
    start_factor = jnp.eye(2 * block_order, dtype=diag_blocks.dtype)
    start_load = jnp.zeros_like(sources[0])
    _, (factors, loads) = lax.scan(forward, (start_factor, start_load), (diag_blocks, embedded, sources))
    next_embeds = jnp.concatenate([embedded[1:], jnp.zeros_like(embedded[:1])], axis=0)

    def backward(upper_value, item):
        factor, load, next_embed = item
        value = apply_inverse(factor, load - times_flipped(upper_value, next_embed))
        return (value, value)
    _, solution = lax.scan(backward, jnp.zeros_like(sources[0]), (factors, loads, next_embeds), reverse=True)
    return solution
```

```python
import jax
import jax.numpy as jnp
from jax import lax
from jax.sharding import PartitionSpec as P
from jax.experimental import pallas as pl
from jax.experimental.pallas import tpu as pltpu

HALF = 64
LANES = 2 * HALF


def dot(left, right, dims=((1,), (0,))):
    return lax.dot_general(
        left,
        right,
        (dims, ((), ())),
        precision=lax.Precision.HIGHEST,
        preferred_element_type=jnp.float32,
    )


def dot_flipped(left, right):
    return dot(left, right, ((1,), (1,)))


def lane_sign(shape):
    lane = lax.broadcasted_iota(jnp.int32, shape, 1)
    return jnp.where(lane % LANES < HALF, -1.0, 1.0).astype(jnp.float32)


def times_i(rows):
    pieces = [
        pltpu.roll(rows[:, start : start + LANES], HALF, 1)
        for start in range(0, rows.shape[1], LANES)
    ]
    turned = pieces[0] if len(pieces) == 1 else jnp.concatenate(pieces, axis=1)
    return turned * lane_sign(turned.shape)


def interleave(rows):
    count = rows.shape[1] // LANES
    pieces = []
    for chunk in range(count):
        pieces.append(rows[:, chunk * HALF : (chunk + 1) * HALF])
        pieces.append(rows[:, (count + chunk) * HALF : (count + chunk + 1) * HALF])
    return jnp.concatenate(pieces, axis=1)


def separate(rows):
    count = rows.shape[1] // LANES
    pieces = [rows[:, 2 * chunk * HALF : (2 * chunk + 1) * HALF] for chunk in range(count)]
    pieces += [rows[:, (2 * chunk + 1) * HALF : (2 * chunk + 2) * HALF] for chunk in range(count)]
    return jnp.concatenate(pieces, axis=1)


def embed(rows):
    turned = times_i(rows)
    pieces = []
    for start in range(0, rows.shape[0], HALF):
        pieces += [rows[start : start + HALF], turned[start : start + HALF]]
    return jnp.concatenate(pieces, axis=0)


def compact(embedded):
    return jnp.concatenate(
        [embedded[start : start + HALF] for start in range(0, embedded.shape[0], LANES)], axis=0
    )


GROUP = 16
TALL = 8


def product(left, right):
    return (left[0] * right[0] - left[1] * right[1], left[0] * right[1] + left[1] * right[0])


def conjugate(value):
    return (value[0], -value[1])


def plus(left, right):
    return (left[0] + right[0], left[1] + right[1])


def minus(left, right):
    return (left[0] - right[0], left[1] - right[1])


def squared(value):
    return value[0] * value[0] + value[1] * value[1]


def scaled_by(value, factor):
    return (value[0] * factor, value[1] * factor)


def invert_pair(head, cross, tail):
    scale = 1.0 / (head * tail - squared(cross))
    return tail * scale, scaled_by(cross, -scale), head * scale


def invert_four(at):
    head = invert_pair(at[0][0][0], at[0][1], at[1][1][0])
    upper = [[at[0][2], at[0][3]], [at[1][2], at[1][3]]]
    mixed = [
        [plus(scaled_by(upper[0][j], head[0]), product(head[1], upper[1][j])) for j in range(2)],
        [
            plus(product(conjugate(head[1]), upper[0][j]), scaled_by(upper[1][j], head[2]))
            for j in range(2)
        ],
    ]

    def schur(i, j):
        return plus(
            product(conjugate(upper[0][i]), mixed[0][j]),
            product(conjugate(upper[1][i]), mixed[1][j]),
        )

    tail = invert_pair(
        at[2][2][0] - schur(0, 0)[0],
        minus(at[2][3], schur(0, 1)),
        at[3][3][0] - schur(1, 1)[0],
    )
    carried = [
        [
            plus(scaled_by(mixed[i][0], tail[0]), product(mixed[i][1], conjugate(tail[1]))),
            plus(product(mixed[i][0], tail[1]), scaled_by(mixed[i][1], tail[2])),
        ]
        for i in range(2)
    ]

    def corner(i, j):
        return plus(
            product(carried[i][0], conjugate(mixed[j][0])),
            product(carried[i][1], conjugate(mixed[j][1])),
        )

    zero = jnp.zeros_like(head[0])
    result = [[None] * 4 for _ in range(4)]
    result[0][0] = (head[0] + corner(0, 0)[0], zero)
    result[0][1] = plus(head[1], corner(0, 1))
    result[1][1] = (head[2] + corner(1, 1)[0], zero)
    result[2][2], result[2][3], result[3][3] = (tail[0], zero), tail[1], (tail[2], zero)
    for i in range(2):
        for j in range(2):
            result[i][2 + j] = (-carried[i][j][0], -carried[i][j][1])
    for i in range(4):
        for j in range(i):
            result[i][j] = conjugate(result[j][i])
    return result


def spread_row(rows, at):
    return jnp.broadcast_to(rows[at : at + 1], (TALL, LANES))


def spread_lane(rows, at):
    return jnp.broadcast_to(rows[:, at : at + 1], (TALL, LANES))


def pick(rows, at):
    return jnp.broadcast_to(rows[at : at + 1], (TALL, LANES))


def total(terms):
    while len(terms) > 1:
        terms = [sum(terms[i : i + 2][1:], terms[i]) for i in range(0, len(terms), 2)]
    return terms[0]


def spread_columns(part, step, count):
    return [(spread_lane(part, step + at), spread_lane(part, step + at + HALF)) for at in range(count)]


def invert_home(panel, spun, work, row_id):
    work = [tuple(jnp.where(row_id >= 0, half, 0.0) for half in value) for value in work]
    diagonal = pick(work[0][0], 0)
    for p in range(TALL):
        here = row_id == p
        real, imag = work[p]
        factor = 1.0 / diagonal
        across = {j: (pick(real, j), pick(imag, j)) for j in range(p + 1, TALL)}
        if p + 1 < TALL:
            diagonal = pick(work[p + 1][0], p + 1) - squared(across[p + 1]) * factor
        real = jnp.where(here, real - 1.0, real)
        imag = jnp.where(here, 0.0, imag)
        for j in range(p + 1, TALL):
            value = (across[j][0] * factor, across[j][1] * -factor)
            work[j] = minus(work[j], product((real, imag), value))
        row, turn = pick(panel, p) * factor, pick(spun, p) * factor
        panel = panel - (real * row + imag * turn)
        spun = spun - (real * turn - imag * row)
    return panel, spun


def invert_group(rows, first, sign, lane, row_id):
    above, below = rows[:TALL], rows[TALL:]
    inside = (lane % HALF >= first) & (lane % HALF < first + TALL)
    after = (lane % HALF >= first + TALL) & (lane % HALF < first + GROUP)
    home = spread_columns(above, first, TALL)
    side = spread_columns(below, first, TALL)
    panel = jnp.where(inside, 0.0, above)
    spun = pltpu.roll(panel, HALF, 1) * sign + jnp.where(lane == first + row_id + HALF, 1.0, 0.0)
    panel = panel + jnp.where(lane == first + row_id, 1.0, 0.0)
    panel, spun = invert_home(panel, spun, home, row_id)
    below = jnp.where(inside, 0.0, below) - total(
        [side[p][0] * pick(panel, p) + side[p][1] * pick(spun, p) for p in range(TALL)]
    )
    step = first + TALL
    home = spread_columns(below, step, TALL)
    side = spread_columns(panel, step, TALL)
    lower = jnp.where(after, 0.0, below)
    turned = pltpu.roll(lower, HALF, 1) * sign + jnp.where(lane == step + row_id + HALF, 1.0, 0.0)
    lower = lower + jnp.where(lane == step + row_id, 1.0, 0.0)
    lower, turned = invert_home(lower, turned, home, row_id)
    rows = [(pick(lower, p), pick(turned, p)) for p in range(TALL)]
    panel = jnp.where(after, 0.0, panel) - total(
        [side[p][0] * rows[p][0] + side[p][1] * rows[p][1] for p in range(TALL)]
    )
    spun = jnp.where(after, 0.0, spun) - total(
        [side[p][0] * rows[p][1] - side[p][1] * rows[p][0] for p in range(TALL)]
    )
    return jnp.concatenate([panel, lower], axis=0), jnp.concatenate([spun, turned], axis=0)


def spread_out(done, spun, first):
    last = HALF - first - GROUP
    before = [jnp.zeros((first, LANES), jnp.float32)] if first else []
    after = [jnp.zeros((last, LANES), jnp.float32)] if last else []
    return jnp.concatenate(before + [done] + after + before + [spun] + after, axis=0)


def invert_small(block):
    lane = lax.broadcasted_iota(jnp.int32, (1, LANES), 1)
    row_id = lax.broadcasted_iota(jnp.int32, (TALL, 1), 0)
    sign = lane_sign((1, LANES))
    group = block[:GROUP]
    for first in range(0, HALF, GROUP):
        done, spun = invert_group(group, first, sign, lane, row_id)
        inside = (lane % HALF >= first) & (lane % HALF < first + GROUP)
        following = first + GROUP
        if following < HALF:
            parts = []
            for start in range(following, following + GROUP, TALL):
                old = block[start : start + TALL]
                columns = spread_columns(old, first, GROUP)
                parts.append(
                    jnp.where(inside, 0.0, old)
                    - total(
                        [
                            columns[at][0] * pick(done, at) + columns[at][1] * pick(spun, at)
                            for at in range(GROUP)
                        ]
                    )
                )
            group = jnp.concatenate(parts, axis=0)
        rest = jnp.where(inside, 0.0, block) - dot(
            jnp.where(inside, block, 0.0), spread_out(done, spun, first)
        )
        above = [rest[:first]] if first else []
        below = [rest[following:]] if following < HALF else []
        block = jnp.concatenate(above + [done] + below, axis=0)
    return block


def invert(ref):
    order = ref.shape[0]

    def step(k, carry):
        rows = pl.ds(pl.multiple_of(k * HALF, HALF), HALF)
        lanes = pl.ds(pl.multiple_of(k * LANES, LANES), LANES)
        small = invert_small(ref[rows, lanes])
        panel = ref[rows, :]
        ref[rows, :] = dot(small, jnp.concatenate([panel, times_i(panel)], axis=0))
        ref[rows, lanes] = small
        fresh = ref[rows, :]
        column = ref[:, lanes]
        ref[:, lanes] = jnp.zeros((order, LANES), jnp.float32)
        ref[...] = ref[...] - dot(column, jnp.concatenate([fresh, times_i(fresh)], axis=0))
        ref[rows, :] = fresh
        return carry

    lax.fori_loop(0, order // HALF, step, 0)


def eliminate(pivot_ref, to_pivot_v, to_pivot_u, block_v, block_u, load_i, load_v, load_u):
    invert(pivot_ref)
    return apply_pivot(
        pivot_ref, to_pivot_v, to_pivot_u, block_v, block_u, load_i, load_v, load_u
    )


def apply_pivot(pivot_ref, to_pivot_v, to_pivot_u, block_v, block_u, load_i, load_v, load_u):
    order, rhs = block_v.shape[0], load_i.shape[0]
    inverse = embed(pivot_ref[...])
    stacked = [compact(to_pivot_v), load_i]
    if to_pivot_u is not None:
        stacked.append(compact(to_pivot_u))
    through = dot(jnp.concatenate(stacked, axis=0), inverse)
    toward_v = dot_flipped(through[: order + rhs], to_pivot_v)
    new_v = jnp.concatenate([block_v, load_v], axis=0) - toward_v
    kept = (through[:order], through[order : order + rhs])
    if to_pivot_u is None:
        return new_v, kept
    toward_u = dot_flipped(through, to_pivot_u)
    new_u = jnp.concatenate([block_u, load_u], axis=0) - jnp.concatenate(
        [toward_u[order + rhs :], toward_u[order : order + rhs]], axis=0
    )
    return new_v, new_u, -toward_u[:order], kept + (through[order + rhs :],)


def flip_where(flip, ref, embedded):
    @pl.when(flip)
    def _():
        ref[...] = embedded.T

    @pl.when(jnp.logical_not(flip))
    def _():
        ref[...] = embedded


def is_left():
    return lax.axis_index("slab") < lax.axis_size("slab") // 2


def invert_kernel(block, inverse):
    inverse[...] = interleave(block[...])
    invert(inverse)


def interior_kernel(
    inverse, boundary, inner, outer, loads,
    new_v, new_u, cross, kept_v, kept_b, kept_u, to_v, to_u,
):
    left = is_left()
    at_interior = jnp.where(left, 0, 1)
    flip_where(left, to_v, embed(interleave(inner[...])))
    flip_where(jnp.logical_not(left), to_u, embed(interleave(outer[...])))
    load_i = interleave(loads[at_interior])
    load_v = interleave(loads[1 - at_interior])
    block_v = interleave(boundary[...])
    zero = jnp.zeros_like(block_v)
    new_v[...], new_u[...], cross[...], kept = apply_pivot(
        inverse, to_v[...], to_u[...], block_v, zero, load_i, load_v, jnp.zeros_like(load_v)
    )
    kept_v[...], kept_b[...], kept_u[...] = kept


def level_kernel(own_v, own_u, own_cross, first_v, new_v, kept_v, kept_b, pivot):
    order = pivot.shape[0]
    joined = first_v[...] + own_u[...]
    pivot[...] = joined[:order]
    new_v[...], kept = eliminate(
        pivot, embed(own_cross[...]), None, own_v[:order], None, joined[order:], own_v[order:], None
    )
    kept_v[...], kept_b[...] = kept


def wide_level_kernel(
    own_v, own_u, own_cross, first_v, first_u, first_cross,
    new_v, new_u, cross, kept_v, kept_b, kept_u, pivot,
):
    order = pivot.shape[0]
    joined = first_v[...] + own_u[...]
    pivot[...] = joined[:order]
    new_v[...], new_u[...], cross[...], kept = eliminate(
        pivot,
        embed(own_cross[...]),
        embed(first_cross[...]).T,
        own_v[:order],
        first_u[:order],
        joined[order:],
        own_v[order:],
        first_u[order:],
    )
    kept_v[...], kept_b[...], kept_u[...] = kept


def center_kernel(own, other, coupling, value, pivot, to_other):
    order = pivot.shape[0]
    flip_where(jnp.logical_not(is_left()), to_other, embed(interleave(coupling[...])))
    pivot[...] = other[:order]
    reduced, _ = eliminate(
        pivot, to_other[...], None, own[:order], None, other[order:], own[order:], None
    )
    pivot[...] = reduced[:order]
    invert(pivot)
    value[...] = dot(reduced[order:], embed(pivot[...]))


def back_kernel(value_v, value_u, kept_v, kept_b, kept_u, middle):
    middle[...] = (
        kept_b[...]
        - dot(value_v[...], embed(kept_v[...]))
        - dot(value_u[...], embed(kept_u[...]))
    )


def narrow_back_kernel(value_v, kept_v, kept_b, middle):
    middle[...] = kept_b[...] - dot(value_v[...], embed(kept_v[...]))


def final_kernel(value_v, value_u, kept_v, kept_b, kept_u, result):
    middle = (
        kept_b[...]
        - dot(value_v[...], embed(kept_v[...]))
        - dot(value_u[...], embed(kept_u[...]))
    )
    at_interior = jnp.where(is_left(), 0, 1)
    result[at_interior] = separate(middle)
    result[1 - at_interior] = separate(value_v[...])


def call(kernel, outs, scratch, *operands, flops=0):
    return pl.pallas_call(
        kernel,
        out_shape=[jax.ShapeDtypeStruct(shape, jnp.float32) for shape in outs],
        scratch_shapes=[pltpu.VMEM(shape, jnp.float32) for shape in scratch],
        cost_estimate=pl.CostEstimate(flops=flops, bytes_accessed=flops // 64, transcendentals=0)
        if flops
        else None,
        compiler_params=pltpu.CompilerParams(vmem_limit_bytes=48 * 1024 * 1024),
    )(*operands)


def gather_columns(shard):
    size = lax.axis_size("orb")
    index = lax.axis_index("orb")
    distance = 1
    while distance < size:
        theirs = lax.ppermute(shard, "orb", [(i, i ^ distance) for i in range(size)])
        first = index // distance % 2 == 0
        shard = jnp.where(
            first,
            jnp.concatenate([shard, theirs], axis=0),
            jnp.concatenate([theirs, shard], axis=0),
        )
        distance *= 2
    return shard


def local(diag_blocks, couplings, sources):
    order, width = couplings.shape[1:]
    rhs = sources.shape[1]
    slabs = lax.axis_size("slab")
    half = slabs // 2
    slab = lax.axis_index("slab")
    left = slab < half
    place = jnp.where(left, slab, slabs - 1 - slab)

    def at(position):
        return (position, slabs - 1 - position)

    shifted = lax.ppermute(couplings[0], "slab", [(i, i - 1) for i in range(half, slabs)])
    interior = gather_columns(jnp.where(left, diag_blocks[0], diag_blocks[1]))
    held = jnp.where(left, diag_blocks[1], diag_blocks[0])
    interior, held = lax.optimization_barrier((interior, held))
    boundary = gather_columns(held)
    outer = jnp.where(left, jnp.where(slab > 0, couplings[0], 0.0), shifted)
    center = jnp.where(left, shifted, couplings[0])
    square, tall, thin, full = (order, width), (order + rhs, width), (rhs, width), (width, width)

    (inverse,) = call(invert_kernel, [square], [], interior, flops=64 * order * width * width)
    new_v, new_u, cross, kept_v, kept_b, kept_u = call(
        interior_kernel,
        [tall, tall, square, square, thin, square],
        [full, full],
        inverse, boundary, couplings[1], outer, sources,
    )
    levels = half.bit_length() - 1
    stored = []
    for level in range(levels):
        distance = 2**level
        firsts = range(distance - 1, half, 2 * distance)
        pairs = [
            (a, b) for first in firsts for a, b in zip(at(first), at(first + distance), strict=True)
        ]
        first_v = lax.ppermute(new_v, "slab", pairs)
        if level == levels - 1:
            new_v, level_v, level_b = call(
                level_kernel, [tall, square, thin], [square], new_v, new_u, cross, first_v
            )
            stored.append((distance, pairs, (level_v, level_b)))
        else:
            first_u = lax.ppermute(new_u, "slab", pairs)
            first_cross = lax.ppermute(cross, "slab", pairs)
            new_v, new_u, cross, level_v, level_b, level_u = call(
                wide_level_kernel,
                [tall, tall, square, square, thin, square],
                [square],
                new_v, new_u, cross, first_v, first_u, first_cross,
            )
            stored.append((distance, pairs, (level_v, level_b, level_u)))
    other = lax.ppermute(new_v, "slab", [(half - 1, half), (half, half - 1)])
    (value_v,) = call(center_kernel, [thin], [square, full], new_v, other, center)
    value_u = jnp.zeros_like(value_v)
    for distance, pairs, kept in reversed(stored):
        if len(kept) == 2:
            (middle,) = call(narrow_back_kernel, [thin], [], value_v, *kept)
        else:
            (middle,) = call(back_kernel, [thin], [], value_v, value_u, *kept)
        sent = lax.ppermute(
            jnp.concatenate([middle, value_u]), "slab", [(b, a) for a, b in pairs]
        )
        is_first = place % (2 * distance) == distance - 1
        value_v = jnp.where(is_first, sent[:rhs], value_v)
        value_u = jnp.where(is_first, sent[rhs:], middle)
    (result,) = call(
        final_kernel, [sources.shape], [], value_v, value_u, kept_v, kept_b, kept_u
    )
    return result


def solution(mesh):
    placed = (
        P(("energy", "slab"), "orb", None),
        P(("energy", "slab"), None, None),
        P(("energy", "slab"), ("orb", "rhs"), None),
    )
    return jax.shard_map(
        local,
        mesh=mesh,
        in_specs=placed,
        out_specs=P(("energy", "slab"), ("orb", "rhs"), None),
        check_vma=False,
    )
```

```python
import jax
import jax.numpy as jnp
from jax import lax
from jax.sharding import PartitionSpec as P
from jax.experimental import pallas as pl
from jax.experimental.pallas import tpu as pltpu

HALF = 64
LANES = 2 * HALF


def dot(left, right, dims=((1,), (0,))):
    return lax.dot_general(
        left,
        right,
        (dims, ((), ())),
        precision=lax.Precision.HIGHEST,
        preferred_element_type=jnp.float32,
    )


def dot_flipped(left, right):
    return dot(left, right, ((1,), (1,)))


def lane_sign(shape):
    lane = lax.broadcasted_iota(jnp.int32, shape, 1)
    return jnp.where(lane % LANES < HALF, -1.0, 1.0).astype(jnp.float32)


def times_i(rows):
    pieces = [
        pltpu.roll(rows[:, start : start + LANES], HALF, 1)
        for start in range(0, rows.shape[1], LANES)
    ]
    turned = pieces[0] if len(pieces) == 1 else jnp.concatenate(pieces, axis=1)
    return turned * lane_sign(turned.shape)


def interleave(rows):
    count = rows.shape[1] // LANES
    pieces = []
    for chunk in range(count):
        pieces.append(rows[:, chunk * HALF : (chunk + 1) * HALF])
        pieces.append(rows[:, (count + chunk) * HALF : (count + chunk + 1) * HALF])
    return jnp.concatenate(pieces, axis=1)


def separate(rows):
    count = rows.shape[1] // LANES
    pieces = [rows[:, 2 * chunk * HALF : (2 * chunk + 1) * HALF] for chunk in range(count)]
    pieces += [rows[:, (2 * chunk + 1) * HALF : (2 * chunk + 2) * HALF] for chunk in range(count)]
    return jnp.concatenate(pieces, axis=1)


def embed(rows):
    turned = times_i(rows)
    pieces = []
    for start in range(0, rows.shape[0], HALF):
        pieces += [rows[start : start + HALF], turned[start : start + HALF]]
    return jnp.concatenate(pieces, axis=0)


def compact(embedded):
    return jnp.concatenate(
        [embedded[start : start + HALF] for start in range(0, embedded.shape[0], LANES)], axis=0
    )


GROUP = 16
TALL = 8


def product(left, right):
    return (left[0] * right[0] - left[1] * right[1], left[0] * right[1] + left[1] * right[0])


def conjugate(value):
    return (value[0], -value[1])


def plus(left, right):
    return (left[0] + right[0], left[1] + right[1])


def minus(left, right):
    return (left[0] - right[0], left[1] - right[1])


def squared(value):
    return value[0] * value[0] + value[1] * value[1]


def scaled_by(value, factor):
    return (value[0] * factor, value[1] * factor)


def invert_pair(head, cross, tail):
    scale = 1.0 / (head * tail - squared(cross))
    return tail * scale, scaled_by(cross, -scale), head * scale


def invert_four(at):
    head = invert_pair(at[0][0][0], at[0][1], at[1][1][0])
    upper = [[at[0][2], at[0][3]], [at[1][2], at[1][3]]]
    mixed = [
        [plus(scaled_by(upper[0][j], head[0]), product(head[1], upper[1][j])) for j in range(2)],
        [
            plus(product(conjugate(head[1]), upper[0][j]), scaled_by(upper[1][j], head[2]))
            for j in range(2)
        ],
    ]

    def schur(i, j):
        return plus(
            product(conjugate(upper[0][i]), mixed[0][j]),
            product(conjugate(upper[1][i]), mixed[1][j]),
        )

    tail = invert_pair(
        at[2][2][0] - schur(0, 0)[0],
        minus(at[2][3], schur(0, 1)),
        at[3][3][0] - schur(1, 1)[0],
    )
    carried = [
        [
            plus(scaled_by(mixed[i][0], tail[0]), product(mixed[i][1], conjugate(tail[1]))),
            plus(product(mixed[i][0], tail[1]), scaled_by(mixed[i][1], tail[2])),
        ]
        for i in range(2)
    ]

    def corner(i, j):
        return plus(
            product(carried[i][0], conjugate(mixed[j][0])),
            product(carried[i][1], conjugate(mixed[j][1])),
        )

    zero = jnp.zeros_like(head[0])
    result = [[None] * 4 for _ in range(4)]
    result[0][0] = (head[0] + corner(0, 0)[0], zero)
    result[0][1] = plus(head[1], corner(0, 1))
    result[1][1] = (head[2] + corner(1, 1)[0], zero)
    result[2][2], result[2][3], result[3][3] = (tail[0], zero), tail[1], (tail[2], zero)
    for i in range(2):
        for j in range(2):
            result[i][2 + j] = (-carried[i][j][0], -carried[i][j][1])
    for i in range(4):
        for j in range(i):
            result[i][j] = conjugate(result[j][i])
    return result


def spread_row(rows, at):
    return jnp.broadcast_to(rows[at : at + 1], (TALL, LANES))


def spread_lane(rows, at):
    return jnp.broadcast_to(rows[:, at : at + 1], (TALL, LANES))


def pick(rows, at):
    return jnp.broadcast_to(rows[at : at + 1], (TALL, LANES))


def total(terms):
    while len(terms) > 1:
        terms = [sum(terms[i : i + 2][1:], terms[i]) for i in range(0, len(terms), 2)]
    return terms[0]


def spread_columns(part, step, count):
    return [(spread_lane(part, step + at), spread_lane(part, step + at + HALF)) for at in range(count)]


def invert_home(panel, spun, work, row_id):
    work = [tuple(jnp.where(row_id >= 0, half, 0.0) for half in value) for value in work]
    diagonal = pick(work[0][0], 0)
    for p in range(TALL):
        here = row_id == p
        real, imag = work[p]
        factor = 1.0 / diagonal
        across = {j: (pick(real, j), pick(imag, j)) for j in range(p + 1, TALL)}
        if p + 1 < TALL:
            diagonal = pick(work[p + 1][0], p + 1) - squared(across[p + 1]) * factor
        real = jnp.where(here, real - 1.0, real)
        imag = jnp.where(here, 0.0, imag)
        for j in range(p + 1, TALL):
            value = (across[j][0] * factor, across[j][1] * -factor)
            work[j] = minus(work[j], product((real, imag), value))
        row, turn = pick(panel, p) * factor, pick(spun, p) * factor
        panel = panel - (real * row + imag * turn)
        spun = spun - (real * turn - imag * row)
    return panel, spun


def invert_group(rows, first, sign, lane, row_id):
    above, below = rows[:TALL], rows[TALL:]
    inside = (lane % HALF >= first) & (lane % HALF < first + TALL)
    after = (lane % HALF >= first + TALL) & (lane % HALF < first + GROUP)
    home = spread_columns(above, first, TALL)
    side = spread_columns(below, first, TALL)
    panel = jnp.where(inside, 0.0, above)
    spun = pltpu.roll(panel, HALF, 1) * sign + jnp.where(lane == first + row_id + HALF, 1.0, 0.0)
    panel = panel + jnp.where(lane == first + row_id, 1.0, 0.0)
    panel, spun = invert_home(panel, spun, home, row_id)
    below = jnp.where(inside, 0.0, below) - total(
        [side[p][0] * pick(panel, p) + side[p][1] * pick(spun, p) for p in range(TALL)]
    )
    step = first + TALL
    home = spread_columns(below, step, TALL)
    side = spread_columns(panel, step, TALL)
    lower = jnp.where(after, 0.0, below)
    turned = pltpu.roll(lower, HALF, 1) * sign + jnp.where(lane == step + row_id + HALF, 1.0, 0.0)
    lower = lower + jnp.where(lane == step + row_id, 1.0, 0.0)
    lower, turned = invert_home(lower, turned, home, row_id)
    rows = [(pick(lower, p), pick(turned, p)) for p in range(TALL)]
    panel = jnp.where(after, 0.0, panel) - total(
        [side[p][0] * rows[p][0] + side[p][1] * rows[p][1] for p in range(TALL)]
    )
    spun = jnp.where(after, 0.0, spun) - total(
        [side[p][0] * rows[p][1] - side[p][1] * rows[p][0] for p in range(TALL)]
    )
    return jnp.concatenate([panel, lower], axis=0), jnp.concatenate([spun, turned], axis=0)


def spread_out(done, spun, first):
    last = HALF - first - GROUP
    before = [jnp.zeros((first, LANES), jnp.float32)] if first else []
    after = [jnp.zeros((last, LANES), jnp.float32)] if last else []
    return jnp.concatenate(before + [done] + after + before + [spun] + after, axis=0)


def invert_small(block, fillers=()):
    lane = lax.broadcasted_iota(jnp.int32, (1, LANES), 1)
    row_id = lax.broadcasted_iota(jnp.int32, (TALL, 1), 0)
    sign = lane_sign((1, LANES))
    group = block[:GROUP]
    fillers = list(fillers)
    slots = HALF // GROUP
    for first in range(0, HALF, GROUP):
        done, spun = invert_group(group, first, sign, lane, row_id)
        inside = (lane % HALF >= first) & (lane % HALF < first + GROUP)
        following = first + GROUP
        if following < HALF:
            parts = []
            for start in range(following, following + GROUP, TALL):
                old = block[start : start + TALL]
                columns = spread_columns(old, first, GROUP)
                parts.append(
                    jnp.where(inside, 0.0, old)
                    - total(
                        [
                            columns[at][0] * pick(done, at) + columns[at][1] * pick(spun, at)
                            for at in range(GROUP)
                        ]
                    )
                )
            group = jnp.concatenate(parts, axis=0)
        rest = jnp.where(inside, 0.0, block) - dot(
            jnp.where(inside, block, 0.0), spread_out(done, spun, first)
        )
        above = [rest[:first]] if first else []
        below = [rest[following:]] if following < HALF else []
        block = jnp.concatenate(above + [done] + below, axis=0)
        share = -(-len(fillers) // slots)
        for filler in fillers[:share]:
            filler()
        fillers, slots = fillers[share:], slots - 1
    return block


def doubled(rows):
    return jnp.concatenate([rows, times_i(rows)], axis=0)


def chunk(rows, at):
    return rows[:, at * LANES : (at + 1) * LANES]


def eliminate(pivot, tail, toward):
    count = pivot.shape[0] // HALF
    blocks = [
        [chunk(pivot[i * HALF : (i + 1) * HALF], k) for k in range(count)] for i in range(count)
    ]
    tails = [chunk(tail, k) for k in range(count)] if tail is not None else None
    scaled = [None] * count
    lower = {}
    sums = [None] * len(toward)
    pending = []

    def bulk(k, inverse, across):
        def rows_below(i):
            def run():
                lower[i, k] = dot(blocks[i][k], inverse)
                change = dot(lower[i, k], across)
                for c in range(k + 1, count):
                    blocks[i][c] = blocks[i][c] - chunk(change, c - k - 1)

            return run

        def scale():
            scaled[k] = dot(tails[k], inverse)

        def shift():
            change = dot(scaled[k], across)
            for c in range(k + 1, count):
                tails[c] = tails[c] - chunk(change, c - k - 1)

        def gather(at):
            def run():
                (first, last), (low, high) = toward[at]
                term = dot_flipped(scaled[k][first:last], embed(tails[k][low:high]))
                sums[at] = term if sums[at] is None else sums[at] + term

            return run

        work = [rows_below(i) for i in range(k + 2, count)] + [scale]
        if k + 1 < count:
            work.append(shift)
        return work + [gather(at) for at in range(len(toward))]

    for k in range(count):
        inverse = doubled(invert_small(blocks[k][k], pending))
        across = None
        if k + 1 < count:
            across = doubled(jnp.concatenate(blocks[k][k + 1 :], axis=1))
            lower[k + 1, k] = dot(blocks[k + 1][k], inverse)
            change = dot(lower[k + 1, k], across)
            for c in range(k + 1, count):
                blocks[k + 1][c] = blocks[k + 1][c] - chunk(change, c - k - 1)
        pending = bulk(k, inverse, across)
    for work in pending:
        work()
    stacked = [lower[i, k] for k in range(count) for i in range(k + 1, count)]
    return jnp.concatenate(scaled, axis=1), jnp.concatenate(stacked, axis=0), sums


def resolve(rows, lower):
    count = rows.shape[1] // LANES
    places = [(i, k) for k in range(count) for i in range(k + 1, count)]
    found = [chunk(rows, k) for k in range(count)]
    for i in range(count - 1, 0, -1):
        for k in range(i):
            at = places.index((i, k)) * HALF
            found[k] = found[k] - dot(found[i], doubled(lower[at : at + HALF]))
    return jnp.concatenate(found, axis=1)


def flip_where(flip, ref, embedded):
    @pl.when(flip)
    def _():
        ref[...] = compact(embedded.T)

    @pl.when(jnp.logical_not(flip))
    def _():
        ref[...] = compact(embedded)


def is_left():
    return lax.axis_index("slab") < lax.axis_size("slab") // 2


def interior_kernel(
    interior, inner, outer, loads, sum_v, new_u, cross, kept_v, kept_b, kept_u, lower, to_v, to_u
):
    left = is_left()
    at_interior = jnp.where(left, 0, 1)
    flip_where(left, to_v, embed(interleave(inner[...])))
    flip_where(jnp.logical_not(left), to_u, embed(interleave(outer[...])))
    load_i = interleave(loads[at_interior])
    order, rhs = to_v.shape[0], load_i.shape[0]
    tail = jnp.concatenate([to_v[...], load_i, to_u[...]], axis=0)
    both, end = order + rhs, 2 * order + rhs
    scaled, lower[...], sums = eliminate(
        interleave(interior[...]), tail, [((0, both), (0, order)), ((0, end), (both, end))]
    )
    sum_v[...] = sums[0]
    new_u[...] = -jnp.concatenate([sums[1][both:], sums[1][order:both]], axis=0)
    cross[...] = -sums[1][:order]
    kept_v[...], kept_b[...], kept_u[...] = scaled[:order], scaled[order:both], scaled[both:]


def boundary_kernel(boundary, loads, sum_v, new_v):
    at_interior = jnp.where(is_left(), 0, 1)
    load_v = interleave(loads[1 - at_interior])
    order = boundary.shape[0]
    new_v[:order] = interleave(boundary[...]) - sum_v[:order]
    new_v[order:] = load_v - sum_v[order:]


def level_kernel(own_v, own_u, own_cross, first_v, new_v, kept_v, kept_b, lower):
    order = own_cross.shape[0]
    joined = first_v[...] + own_u[...]
    tail = jnp.concatenate([own_cross[...], joined[order:]], axis=0)
    scaled, lower[...], sums = eliminate(joined[:order], tail, [((0, tail.shape[0]), (0, order))])
    new_v[...] = own_v[...] - sums[0]
    kept_v[...], kept_b[...] = scaled[:order], scaled[order:]


def wide_level_kernel(
    own_v, own_u, own_cross, first_v, first_u, first_cross,
    new_v, new_u, cross, kept_v, kept_b, kept_u, lower,
):
    order = own_cross.shape[0]
    joined = first_v[...] + own_u[...]
    tail = jnp.concatenate(
        [own_cross[...], joined[order:], compact(embed(first_cross[...]).T)], axis=0
    )
    both, end = joined.shape[0], tail.shape[0]
    scaled, lower[...], sums = eliminate(
        joined[:order], tail, [((0, both), (0, order)), ((0, end), (both, end))]
    )
    new_v[...] = own_v[...] - sums[0]
    new_u[...] = first_u[...] - jnp.concatenate([sums[1][both:], sums[1][order:both]], axis=0)
    cross[...] = -sums[1][:order]
    kept_v[...], kept_b[...], kept_u[...] = scaled[:order], scaled[order:both], scaled[both:]


PIECES = 2


def greet(partners):
    barrier = pltpu.get_barrier_semaphore()
    for partner in partners:
        pl.semaphore_signal(barrier, inc=1, device_id=partner, device_id_type=pl.DeviceIdType.MESH)
    pl.semaphore_wait(barrier, len(partners))


def siblings():
    size = lax.axis_size("rhs")
    return [{"rhs": lax.rem(lax.axis_index("rhs") + step, size)} for step in range(1, size)]


def remote(source, target, send, receive, device):
    return pltpu.make_async_remote_copy(
        src_ref=source, dst_ref=target, send_sem=send, recv_sem=receive,
        device_id=device, device_id_type=pl.DeviceIdType.MESH,
    )


class Relay:
    def __init__(self, source, target, device, order, sems):
        self.source, self.target, self.device, self.order = source, target, device, order
        self.send, self.receive, self.pass_send, self.pass_receive = sems
        self.cores = lax.axis_size("rhs")
        self.piece = order // self.cores // PIECES

    def rows(self, core, piece):
        start = (core * PIECES + piece) * self.piece
        return pl.ds(pl.multiple_of(start, 8), self.piece)

    def copies(self):
        core = lax.axis_index("rhs")
        own = [
            remote(
                self.source.at[self.rows(core, piece)], self.target.at[self.rows(core, piece)],
                self.send.at[piece], self.receive.at[piece], self.device,
            )
            for piece in range(PIECES)
        ]
        after = pl.ds(self.order, self.source.shape[0] - self.order)
        own.append(
            remote(
                self.source.at[after], self.target.at[after],
                self.send.at[PIECES], self.receive.at[PIECES], self.device,
            )
        )
        return own

    def passes(self, piece):
        core = lax.axis_index("rhs")
        rows = self.rows(core, piece)
        return [
            remote(
                self.target.at[rows], self.target.at[rows],
                self.pass_send.at[piece, step], self.pass_receive.at[piece, step], device,
            )
            for step, device in enumerate(siblings())
        ]

    def start(self):
        for copy in self.copies():
            copy.start()

    def wait_sent(self):
        for copy in self.copies():
            copy.wait_send()

    def wait_received(self):
        arrived = self.copies()
        for piece in range(PIECES):
            arrived[piece].wait_recv()
            for copy in self.passes(piece):
                copy.start()
        arrived[PIECES].wait_recv()
        for piece in range(PIECES):
            for copy in self.passes(piece):
                copy.wait()


def relay_semaphores():
    passing = (PIECES, max(1, lax.axis_size("rhs") - 1))
    return [
        pltpu.SemaphoreType.DMA((PIECES + 1,)), pltpu.SemaphoreType.DMA((PIECES + 1,)),
        pltpu.SemaphoreType.DMA(passing), pltpu.SemaphoreType.DMA(passing),
    ]


def center_kernel(own, coupling, value, other, to_other, *sems):
    order = coupling.shape[0]
    half = lax.axis_size("slab") // 2
    slab = lax.axis_index("slab")
    left = is_left()
    middle = (slab == half - 1) | (slab == half)

    @pl.when(middle)
    def _():
        partner = {"slab": jnp.where(left, half, half - 1)}
        greet([partner] + siblings())
        relay = Relay(own, other, partner, order, sems)
        relay.start()
        flip_where(jnp.logical_not(left), to_other, embed(interleave(coupling[...])))
        relay.wait_received()
        tail = jnp.concatenate([to_other[...], other[order:]], axis=0)
        _, _, sums = eliminate(other[:order], tail, [((0, tail.shape[0]), (0, order))])
        reduced = own[...] - sums[0]
        scaled, lower, _ = eliminate(reduced[:order], reduced[order:], [])
        value[...] = resolve(scaled, lower)
        relay.wait_sent()

    @pl.when(jnp.logical_not(middle))
    def _():
        value[...] = jnp.zeros(value.shape, jnp.float32)


def back_kernel(value_v, value_u, kept_v, kept_b, kept_u, lower, middle):
    found = (
        kept_b[...]
        - dot(value_v[...], embed(kept_v[...]))
        - dot(value_u[...], embed(kept_u[...]))
    )
    middle[...] = resolve(found, lower[...])


def narrow_back_kernel(value_v, kept_v, kept_b, lower, middle):
    middle[...] = resolve(kept_b[...] - dot(value_v[...], embed(kept_v[...])), lower[...])


def final_kernel(value_v, value_u, kept_v, kept_b, kept_u, lower, result):
    found = (
        kept_b[...]
        - dot(value_v[...], embed(kept_v[...]))
        - dot(value_u[...], embed(kept_u[...]))
    )
    at_interior = jnp.where(is_left(), 0, 1)
    result[at_interior] = separate(resolve(found, lower[...]))
    result[1 - at_interior] = separate(value_v[...])


def call(kernel, outs, scratch, *operands, flops=0, collective_id=None):
    return pl.pallas_call(
        kernel,
        out_shape=[jax.ShapeDtypeStruct(shape, jnp.float32) for shape in outs],
        scratch_shapes=[
            pltpu.VMEM(shape, jnp.float32) if isinstance(shape, tuple) else shape
            for shape in scratch
        ],
        cost_estimate=pl.CostEstimate(flops=flops, bytes_accessed=flops // 64, transcendentals=0)
        if flops
        else None,
        compiler_params=pltpu.CompilerParams(
            vmem_limit_bytes=48 * 1024 * 1024,
            collective_id=collective_id,
            has_side_effects=collective_id is not None,
        ),
    )(*operands)


def gather_columns(shard):
    size = lax.axis_size("orb")
    index = lax.axis_index("orb")
    distance = 1
    while distance < size:
        theirs = lax.ppermute(shard, "orb", [(i, i ^ distance) for i in range(size)])
        first = index // distance % 2 == 0
        shard = jnp.where(
            first,
            jnp.concatenate([shard, theirs], axis=0),
            jnp.concatenate([theirs, shard], axis=0),
        )
        distance *= 2
    return shard


def local(diag_blocks, couplings, sources):
    order, width = couplings.shape[1:]
    rhs = sources.shape[1]
    slabs = lax.axis_size("slab")
    half = slabs // 2
    slab = lax.axis_index("slab")
    left = slab < half
    place = jnp.where(left, slab, slabs - 1 - slab)

    def at(position):
        return (position, slabs - 1 - position)

    shifted = lax.ppermute(couplings[0], "slab", [(i, i - 1) for i in range(half, slabs)])
    interior = gather_columns(jnp.where(left, diag_blocks[0], diag_blocks[1]))
    held = jnp.where(left, diag_blocks[1], diag_blocks[0])
    interior, held = lax.optimization_barrier((interior, held))
    boundary = gather_columns(held)
    outer = jnp.where(left, jnp.where(slab > 0, couplings[0], 0.0), shifted)
    center = jnp.where(left, shifted, couplings[0])
    square, tall, thin = (order, width), (order + rhs, width), (rhs, width)
    count = order // HALF
    below = (count * (count - 1) // 2 * HALF, LANES)

    sum_v, new_u, cross, kept_v, kept_b, kept_u, lower = call(
        interior_kernel,
        [tall, tall, square, square, thin, square, below],
        [square, square],
        interior, couplings[1], outer, sources, flops=64 * order * width * width,
    )
    (new_v,) = call(boundary_kernel, [tall], [], boundary, sources, sum_v)
    levels = half.bit_length() - 1
    stored = []
    for level in range(levels):
        distance = 2**level
        firsts = range(distance - 1, half, 2 * distance)
        pairs = [
            (a, b) for first in firsts for a, b in zip(at(first), at(first + distance), strict=True)
        ]
        first_v = lax.ppermute(new_v, "slab", pairs)
        if level == levels - 1:
            new_v, level_v, level_b, level_l = call(
                level_kernel, [tall, square, thin, below], [], new_v, new_u, cross, first_v
            )
            stored.append((distance, pairs, (level_v, level_b, level_l)))
        else:
            first_u = lax.ppermute(new_u, "slab", pairs)
            first_cross = lax.ppermute(cross, "slab", pairs)
            new_v, new_u, cross, level_v, level_b, level_u, level_l = call(
                wide_level_kernel,
                [tall, tall, square, square, thin, square, below],
                [],
                new_v, new_u, cross, first_v, first_u, first_cross,
            )
            stored.append((distance, pairs, (level_v, level_b, level_u, level_l)))
    (value_v,) = call(
        center_kernel,
        [thin],
        [pltpu.VMEM(tall, jnp.float32), pltpu.VMEM(square, jnp.float32), *relay_semaphores()],
        new_v, center, collective_id=1,
    )
    value_u = jnp.zeros_like(value_v)
    for distance, pairs, kept in reversed(stored):
        if len(kept) == 3:
            (middle,) = call(narrow_back_kernel, [thin], [], value_v, *kept)
        else:
            (middle,) = call(back_kernel, [thin], [], value_v, value_u, *kept)
        sent = lax.ppermute(
            jnp.concatenate([middle, value_u]), "slab", [(b, a) for a, b in pairs]
        )
        is_first = place % (2 * distance) == distance - 1
        value_v = jnp.where(is_first, sent[:rhs], value_v)
        value_u = jnp.where(is_first, sent[rhs:], middle)
    (result,) = call(
        final_kernel, [sources.shape], [], value_v, value_u, kept_v, kept_b, kept_u, lower
    )
    return result


def solution(mesh):
    placed = (
        P(("energy", "slab"), "orb", None),
        P(("energy", "slab"), None, None),
        P(("energy", "slab"), ("orb", "rhs"), None),
    )
    return jax.shard_map(
        local,
        mesh=mesh,
        in_specs=placed,
        out_specs=P(("energy", "slab"), ("orb", "rhs"), None),
        check_vma=False,
    )
```

```python
import functools
import types

import jax
import jax.numpy as jnp
from jax import lax
from jax.sharding import PartitionSpec as P
from jax.experimental import pallas as pl
from jax.experimental.pallas import tpu as pltpu

HALF = 64
LANES = 2 * HALF


def dot(left, right, dims=((1,), (0,))):
    return lax.dot_general(
        left,
        right,
        (dims, ((), ())),
        precision=lax.Precision.HIGHEST,
        preferred_element_type=jnp.float32,
    )


def dot_flipped(left, right):
    return dot(left, right, ((1,), (1,)))


def lane_sign(shape):
    lane = lax.broadcasted_iota(jnp.int32, shape, 1)
    return jnp.where(lane % LANES < HALF, -1.0, 1.0).astype(jnp.float32)


def times_i(rows):
    pieces = [
        pltpu.roll(rows[:, start : start + LANES], HALF, 1)
        for start in range(0, rows.shape[1], LANES)
    ]
    turned = pieces[0] if len(pieces) == 1 else jnp.concatenate(pieces, axis=1)
    return turned * lane_sign(turned.shape)


def interleave(rows):
    count = rows.shape[1] // LANES
    pieces = []
    for chunk in range(count):
        pieces.append(rows[:, chunk * HALF : (chunk + 1) * HALF])
        pieces.append(rows[:, (count + chunk) * HALF : (count + chunk + 1) * HALF])
    return jnp.concatenate(pieces, axis=1)


def separate(rows):
    count = rows.shape[1] // LANES
    pieces = [rows[:, 2 * chunk * HALF : (2 * chunk + 1) * HALF] for chunk in range(count)]
    pieces += [rows[:, (2 * chunk + 1) * HALF : (2 * chunk + 2) * HALF] for chunk in range(count)]
    return jnp.concatenate(pieces, axis=1)


def embed(rows):
    turned = times_i(rows)
    pieces = []
    for start in range(0, rows.shape[0], HALF):
        pieces += [rows[start : start + HALF], turned[start : start + HALF]]
    return jnp.concatenate(pieces, axis=0)


def compact(embedded):
    return jnp.concatenate(
        [embedded[start : start + HALF] for start in range(0, embedded.shape[0], LANES)], axis=0
    )


GROUP = 16
TALL = 8


def product(left, right):
    return (left[0] * right[0] - left[1] * right[1], left[0] * right[1] + left[1] * right[0])


def minus(left, right):
    return (left[0] - right[0], left[1] - right[1])


def squared(value):
    return value[0] * value[0] + value[1] * value[1]


def spread_lane(rows, at):
    return jnp.broadcast_to(rows[:, at : at + 1], (TALL, LANES))


def pick(rows, at):
    return jnp.broadcast_to(rows[at : at + 1], (TALL, LANES))


def total(terms):
    while len(terms) > 1:
        terms = [sum(terms[i : i + 2][1:], terms[i]) for i in range(0, len(terms), 2)]
    return terms[0]


def spread_columns(part, step, count):
    return [(spread_lane(part, step + at), spread_lane(part, step + at + HALF)) for at in range(count)]


def invert_home(panel, spun, work, row_id):
    work = [tuple(jnp.where(row_id >= 0, half, 0.0) for half in value) for value in work]
    diagonal = pick(work[0][0], 0)
    for p in range(TALL):
        here = row_id == p
        real, imag = work[p]
        factor = 1.0 / diagonal
        across = {j: (pick(real, j), pick(imag, j)) for j in range(p + 1, TALL)}
        if p + 1 < TALL:
            diagonal = pick(work[p + 1][0], p + 1) - squared(across[p + 1]) * factor
        real = jnp.where(here, real - 1.0, real)
        imag = jnp.where(here, 0.0, imag)
        for j in range(p + 1, TALL):
            value = (across[j][0] * factor, across[j][1] * -factor)
            work[j] = minus(work[j], product((real, imag), value))
        row, turn = pick(panel, p) * factor, pick(spun, p) * factor
        panel = panel - (real * row + imag * turn)
        spun = spun - (real * turn - imag * row)
    return panel, spun


def invert_group(rows, first, sign, lane, row_id):
    above, below = rows[:TALL], rows[TALL:]
    inside = (lane % HALF >= first) & (lane % HALF < first + TALL)
    after = (lane % HALF >= first + TALL) & (lane % HALF < first + GROUP)
    home = spread_columns(above, first, TALL)
    side = spread_columns(below, first, TALL)
    panel = jnp.where(inside, 0.0, above)
    spun = pltpu.roll(panel, HALF, 1) * sign + jnp.where(lane == first + row_id + HALF, 1.0, 0.0)
    panel = panel + jnp.where(lane == first + row_id, 1.0, 0.0)
    panel, spun = invert_home(panel, spun, home, row_id)
    below = jnp.where(inside, 0.0, below) - total(
        [side[p][0] * pick(panel, p) + side[p][1] * pick(spun, p) for p in range(TALL)]
    )
    step = first + TALL
    home = spread_columns(below, step, TALL)
    side = spread_columns(panel, step, TALL)
    lower = jnp.where(after, 0.0, below)
    turned = pltpu.roll(lower, HALF, 1) * sign + jnp.where(lane == step + row_id + HALF, 1.0, 0.0)
    lower = lower + jnp.where(lane == step + row_id, 1.0, 0.0)
    lower, turned = invert_home(lower, turned, home, row_id)
    rows = [(pick(lower, p), pick(turned, p)) for p in range(TALL)]
    panel = jnp.where(after, 0.0, panel) - total(
        [side[p][0] * rows[p][0] + side[p][1] * rows[p][1] for p in range(TALL)]
    )
    spun = jnp.where(after, 0.0, spun) - total(
        [side[p][0] * rows[p][1] - side[p][1] * rows[p][0] for p in range(TALL)]
    )
    return jnp.concatenate([panel, lower], axis=0), jnp.concatenate([spun, turned], axis=0)


def spread_out(done, spun, first):
    last = HALF - first - GROUP
    before = [jnp.zeros((first, LANES), jnp.float32)] if first else []
    after = [jnp.zeros((last, LANES), jnp.float32)] if last else []
    return jnp.concatenate(before + [done] + after + before + [spun] + after, axis=0)


def invert_small(block, fillers=()):
    lane = lax.broadcasted_iota(jnp.int32, (1, LANES), 1)
    row_id = lax.broadcasted_iota(jnp.int32, (TALL, 1), 0)
    sign = lane_sign((1, LANES))
    group = block[:GROUP]
    fillers = list(fillers)
    slots = HALF // GROUP
    for first in range(0, HALF, GROUP):
        done, spun = invert_group(group, first, sign, lane, row_id)
        inside = (lane % HALF >= first) & (lane % HALF < first + GROUP)
        following = first + GROUP
        if following < HALF:
            parts = []
            for start in range(following, following + GROUP, TALL):
                old = block[start : start + TALL]
                columns = spread_columns(old, first, GROUP)
                parts.append(
                    jnp.where(inside, 0.0, old)
                    - total(
                        [
                            columns[at][0] * pick(done, at) + columns[at][1] * pick(spun, at)
                            for at in range(GROUP)
                        ]
                    )
                )
            group = jnp.concatenate(parts, axis=0)
        rest = jnp.where(inside, 0.0, block) - dot(
            jnp.where(inside, block, 0.0), spread_out(done, spun, first)
        )
        above = [rest[:first]] if first else []
        below = [rest[following:]] if following < HALF else []
        block = jnp.concatenate(above + [done] + below, axis=0)
        share = -(-len(fillers) // slots)
        for filler in fillers[:share]:
            filler()
        fillers, slots = fillers[share:], slots - 1
    return block


def doubled(rows):
    return jnp.concatenate([rows, times_i(rows)], axis=0)


def hermitian(block):
    return doubled(block).T[:HALF]


def chunk(rows, at):
    return rows[:, at * LANES : (at + 1) * LANES]


def chunks(rows):
    return [chunk(rows, at) for at in range(rows.shape[1] // LANES)]


def added(total_so_far, term):
    return term if total_so_far is None else total_so_far + term


def eliminate(count, block, tails, toward, before=None, keep=None):
    tails = list(tails)
    scaled = [None] * count
    lower = {}
    changes = {}
    sums = [None] * len(toward)
    pending = []

    def bulk(k, inverse, across, heads):
        def row_below(i):
            def run():
                lower[i, k] = dot(heads[i], inverse)
                change = dot(lower[i, k], across[:, (i - k - 1) * LANES :])
                for c in range(i, count):
                    changes[i, c] = added(changes.get((i, c)), chunk(change, c - i))

            return run

        def scale():
            scaled[k] = dot(tails[k], inverse)

        def shift():
            change = dot(scaled[k], across)
            for c in range(k + 1, count):
                tails[c] = tails[c] - chunk(change, c - k - 1)

        def gather(at):
            def run():
                (first, last), (low, high) = toward[at]
                term = dot_flipped(scaled[k][first:last], embed(tails[k][low:high]))
                sums[at] = added(sums[at], term)

            return run

        work = [row_below(i) for i in range(k + 2, count)] + [scale]
        if k + 1 < count:
            work.append(shift)
        return work + [gather(at) for at in range(len(toward))]

    for k in range(count):
        if before is not None:
            before(k)
        row = [
            block(k, c) - changes[k, c] if (k, c) in changes else block(k, c)
            for c in range(k, count)
        ]
        across, heads = None, {}
        if k + 1 < count:
            across = doubled(jnp.concatenate(row[1:], axis=1))
            heads = {i: hermitian(row[i - k]) for i in range(k + 1, count)}
        inverse = doubled(invert_small(row[0], pending))
        if k + 1 < count:
            lower[k + 1, k] = dot(heads[k + 1], inverse)
            change = dot(lower[k + 1, k], across)
            for c in range(k + 1, count):
                changes[k + 1, c] = added(changes.get((k + 1, c)), chunk(change, c - k - 1))
        if keep is not None:
            keep(k, inverse, across)
        pending = bulk(k, inverse, across, heads)
    for work in pending:
        work()
    stacked = [lower[i, k] for k in range(count) for i in range(k + 1, count)]
    return jnp.concatenate(scaled, axis=1), jnp.concatenate(stacked, axis=0), sums


def resolve(rows, lower):
    count = rows.shape[1] // LANES
    places = [(i, k) for k in range(count) for i in range(k + 1, count)]
    found = chunks(rows)
    for i in range(count - 1, 0, -1):
        for k in range(i):
            at = places.index((i, k)) * HALF
            found[k] = found[k] - dot(found[i], doubled(lower[at : at + HALF]))
    return jnp.concatenate(found, axis=1)


def blocks_of(*refs):
    def block(i, c):
        rows, lanes = slice(i * HALF, (i + 1) * HALF), slice(c * LANES, (c + 1) * LANES)
        value = refs[0][rows, lanes]
        for ref in refs[1:]:
            value = value + ref[rows, lanes]
        return value

    return block


def remote(source, target, send, receive, device):
    return pltpu.make_async_remote_copy(
        src_ref=source, dst_ref=target, send_sem=send, recv_sem=receive,
        device_id=device, device_id_type=pl.DeviceIdType.MESH,
    )


def siblings():
    size = lax.axis_size("rhs")
    return [{"rhs": lax.rem(lax.axis_index("rhs") + step, size)} for step in range(1, size)]


class Relay:
    def __init__(self, source, target, device, order, sems):
        self.source, self.target, self.device, self.order = source, target, device, order
        self.send, self.receive, self.pass_send, self.pass_receive = sems
        self.share = HALF // lax.axis_size("rhs")
        self.count = order // HALF

    def part(self, ref, core, piece):
        start = piece * HALF + core * self.share
        rows = pl.ds(pl.multiple_of(start, 8), self.share)
        return ref.at[rows, piece * LANES :]

    def copy(self, piece):
        if piece == self.count:
            after = pl.ds(self.order, self.source.shape[0] - self.order)
            source, target = self.source.at[after], self.target.at[after]
        else:
            core = lax.axis_index("rhs")
            source, target = (self.part(ref, core, piece) for ref in (self.source, self.target))
        return remote(
            source, target, self.send.at[piece], self.receive.at[piece], self.device
        )

    def passes(self, piece):
        part = self.part(self.target, lax.axis_index("rhs"), piece)
        return [
            remote(part, part, self.pass_send.at[piece, step], self.pass_receive.at[piece, step], to)
            for step, to in enumerate(siblings())
        ]

    def start(self):
        for piece in range(self.count + 1):
            self.copy(piece).start()

    def wait_sent(self):
        for piece in range(self.count + 1):
            self.copy(piece).wait_send()

    def wait_received(self):
        for piece in range(self.count):
            self.copy(piece).wait_recv()
            for copy in self.passes(piece):
                copy.start()
        self.copy(self.count).wait_recv()
        for piece in range(self.count):
            for copy in self.passes(piece):
                copy.wait()


def relay_semaphores(count):
    passing = (count, max(1, lax.axis_size("rhs") - 1))
    return [
        pltpu.SemaphoreType.DMA((count + 1,)), pltpu.SemaphoreType.DMA((count + 1,)),
        pltpu.SemaphoreType.DMA(passing), pltpu.SemaphoreType.DMA(passing),
    ]


def flipped_where(flip, ref, rows):
    @pl.when(flip)
    def _():
        ref[...] = compact(embed(rows).T)

    @pl.when(jnp.logical_not(flip))
    def _():
        ref[...] = rows


def reversed_where(flip, rows):
    pieces = chunks(rows)
    return jnp.where(flip, jnp.concatenate(pieces[::-1], axis=1), rows)


def solve_kernel(tree, diag, couplings, sources, result, *refs):
    at = types.SimpleNamespace(**jax.tree.unflatten(tree, refs))
    order, width = couplings.shape[1:]
    shard, rhs = diag.shape[1], sources.shape[1]
    count = order // HALF
    both = order + rhs
    slabs, orbs = lax.axis_size("slab"), lax.axis_size("orb")
    half = slabs // 2
    levels = half.bit_length() - 1
    slab, orb = lax.axis_index("slab"), lax.axis_index("orb")
    left = slab < half
    place = jnp.where(left, slab, slabs - 1 - slab)
    middle = place == half - 1
    inward = jnp.where(left, 1, -1)
    at_interior = jnp.where(left, 0, 1)
    paired = orbs == 2 and 2 * shard == 3 * HALF and order == 2 * shard
    turned = orb == 1 if paired else jnp.bool_(False)

    fetches = [
        pltpu.make_async_copy(ref, held, at.fetch.at[i])
        for i, (ref, held) in enumerate(((diag, at.diag), (sources, at.load), (couplings, at.coupling)))
    ]
    for fetch in fetches:
        fetch.start()
    barrier = pltpu.get_barrier_semaphore()

    def greet(device):
        pl.semaphore_signal(barrier, inc=1, device_id=device, device_id_type=pl.DeviceIdType.MESH)

    peers = [lax.rem(orb + step, orbs) for step in range(1, orbs)]
    owners = [lax.rem(orb + orbs - step, orbs) for step in range(1, orbs)]
    for device in [{"orb": peer} for peer in peers] + siblings():
        greet(device)
    expected = len(peers) + lax.axis_size("rhs") - 1
    for distance in sorted({1, *(2**level for level in range(levels))}):
        for other in (slab - distance, slab + distance):
            inside = (other >= 0) & (other < slabs)
            expected = expected + jnp.where(inside, 1, 0)
            pl.when(inside)(lambda other=other: greet({"slab": other}))
    fetches[0].wait()
    pl.semaphore_wait(barrier, expected)

    def rows_from(owner, low, size):
        return pl.ds(pl.multiple_of(owner * shard + low, 8), size)

    extra = shard - HALF
    if paired:
        def spans(owner):
            first = owner == 0
            return [(jnp.where(first, HALF, 0), extra), (jnp.where(first, 0, extra), HALF)]
    else:
        def spans(owner):
            return [(0, shard)]

    def gather_copies(gathered, layer, owner, step, device, first_sem, parts):
        return [
            remote(
                at.diag.at[layer, pl.ds(pl.multiple_of(low, 8), size)],
                gathered.at[rows_from(owner, low, size)],
                at.orb_send.at[first_sem + piece, step],
                at.orb_receive.at[first_sem + piece, step],
                device,
            )
            for piece, (low, size) in enumerate(parts)
        ]

    pieces = len(spans(orb))
    sent = []
    for step, peer in enumerate(peers):
        sent += gather_copies(
            at.interior, at_interior, orb, step, {"orb": peer}, 0, spans(orb)
        )
    for step, peer in enumerate(peers):
        sent += gather_copies(
            at.boundary, 1 - at_interior, orb, step, {"orb": peer}, pieces, [(0, shard)]
        )
    for copy in sent:
        copy.start()

    def wait_interior(piece):
        for step, owner in enumerate(owners):
            low, size = spans(owner)[piece]
            gather_copies(
                at.interior, at_interior, owner, step, {"orb": owner}, 0, spans(owner)
            )[piece].wait_recv()
            rows = rows_from(owner, low, size)
            at.pivot[rows] = interleave(at.interior[rows])

    def wait_boundary():
        for step, owner in enumerate(owners):
            gather_copies(
                at.boundary, 1 - at_interior, owner, step, {"orb": owner}, pieces, [(0, shard)]
            )[0].wait_recv()
        at.boundary[rows_from(orb, 0, shard)] = at.diag[1 - at_interior]

    fetches[1].wait()
    fetches[2].wait()
    shift = remote(
        at.coupling.at[0], at.shifted, at.shift.at[0], at.shift.at[1],
        {"slab": jnp.where(slab > 0, slab - 1, 1)},
    )
    shifts = slab >= half
    pl.when(shifts)(shift.start)

    def place_of(position):
        return jnp.where(turned, count - 1 - position, position)

    def pivot_block(i, c):
        rows = pl.ds(pl.multiple_of(place_of(i) * HALF, HALF), HALF)
        return at.pivot[rows, pl.ds(pl.multiple_of(place_of(c) * LANES, LANES), LANES)]

    at.pivot[rows_from(orb, 0, shard)] = interleave(at.diag[at_interior])
    flipped_where(left, at.to_v, interleave(at.coupling[1]))
    tail = jnp.concatenate([at.to_v[...], interleave(at.load[at_interior])], axis=0)

    def before(k):
        if paired and k > 0:
            wait_interior(k - 1)
        elif not paired and k == 0:
            wait_interior(0)

    def keep(k, inverse, across):
        at.inverse[k] = inverse
        if across is not None:
            at.across[k, :, : across.shape[1]] = across

    scaled, lower, sums = eliminate(
        count, pivot_block, chunks(reversed_where(turned, tail)), [((0, both), (0, order))],
        before, keep,
    )
    at.kept[:both] = scaled
    at.lower[...] = lower
    wait_boundary()
    own_v, own_u, cross = at.own_v, at.own_u, at.cross
    own_v[:order] = interleave(at.boundary[...]) - sums[0][:order]
    own_v[order:] = interleave(at.load[1 - at_interior]) - sums[0][order:]

    def relay(level, source, target, device):
        return Relay(source, target, device, order, at.relay[level])

    def outward():
        outer = at.outer

        @pl.when(left)
        def _():
            outer[...] = interleave(at.coupling[0])

        @pl.when(jnp.logical_not(left))
        def _():
            shift.wait_recv()
            outer[...] = compact(embed(interleave(at.shifted[...])).T)

        tails = chunks(reversed_where(turned, outer[...]))
        total_u = None
        for k in range(count):
            found = dot(tails[k], at.inverse[k])
            if k + 1 < count:
                change = dot(found, at.across[k, :, : (count - 1 - k) * LANES])
                for c in range(k + 1, count):
                    tails[c] = tails[c] - chunk(change, c - k - 1)
            lanes = slice(k * LANES, (k + 1) * LANES)
            at.kept[both:, lanes] = found
            stacked = jnp.concatenate([at.kept[:both, lanes], found], axis=0)
            total_u = added(total_u, dot_flipped(stacked, embed(tails[k])))
        own_u[:order] = -total_u[both:]
        own_u[order:] = -total_u[order:both]
        cross[...] = -total_u[:order]

    def no_outward():
        own_u[...] = jnp.zeros(own_u.shape, jnp.float32)
        cross[...] = jnp.zeros(cross.shape, jnp.float32)
        at.kept[both:] = jnp.zeros((order, width), jnp.float32)

    def settle():
        at.kept[...] = resolve(at.kept[...], at.lower[...])

    def settle_levels(below):
        for level in range(below):
            kept = at.level_kept[level]
            kept[...] = resolve(kept[...], at.level_lower[level][...])

    finish = []
    for level in range(levels):
        distance = 2**level
        wide = level < levels - 1
        sends = lax.rem(place, 2 * distance) == distance - 1
        takes = lax.rem(place, 2 * distance) == 2 * distance - 1
        device = {"slab": jnp.where(sends, slab + inward * distance, slab - inward * distance)}
        first_v = at.first_v[level]
        move = relay(level, own_v, first_v, device)
        pl.when(sends)(move.start)
        if level == 0:
            pl.when(place > 0)(outward)
            pl.when(place == 0)(no_outward)
        extras = []
        if wide:
            extras = [
                remote(
                    ref, target,
                    at.extra_send[level].at[i], at.extra_receive[level].at[i], device,
                )
                for i, (ref, target) in enumerate(
                    ((own_u, at.first_u[level]), (cross, at.first_cross[level]))
                )
            ]
            for copy in extras:
                pl.when(sends)(copy.start)
        kept, level_lower = at.level_kept[level], at.level_lower[level]

        @pl.when(sends)
        def _(level=level):
            settle()
            settle_levels(level)

        @pl.when(takes)
        def _(level=level, wide=wide, move=move, extras=extras, first_v=first_v, kept=kept, level_lower=level_lower):
            move.wait_received()
            for copy in extras:
                copy.wait_recv()
            load = first_v[order:] + own_u[order:]
            parts = [cross[...], load]
            toward = [((0, both), (0, order))]
            if wide:
                parts.append(compact(embed(at.first_cross[level][...]).T))
                toward.append(((0, both + order), (both, both + order)))
            tail = jnp.concatenate(parts, axis=0)
            scaled, lower, sums = eliminate(count, blocks_of(first_v, own_u), chunks(tail), toward)
            kept[...] = scaled
            level_lower[...] = lower
            own_v[...] = own_v[...] - sums[0]
            if wide:
                first_u = at.first_u[level]
                own_u[:order] = first_u[:order] - sums[1][both:]
                own_u[order:] = first_u[order:] - sums[1][order:both]
                cross[...] = -sums[1][:order]

        def sent_all(move=move, extras=extras):
            move.wait_sent()
            for copy in extras:
                copy.wait_send()

        finish.append((sends, sent_all))

    value_v, value_u = at.value_v, at.value_u
    value_u[...] = jnp.zeros(value_u.shape, jnp.float32)
    swap = relay(levels, own_v, at.other, {"slab": jnp.where(left, half, half - 1)})

    @pl.when(middle)
    def _():
        swap.start()
        settle_levels(levels)

        @pl.when(left)
        def _():
            shift.wait_recv()
            at.to_other[...] = interleave(at.shifted[...])

        @pl.when(jnp.logical_not(left))
        def _():
            at.to_other[...] = compact(embed(interleave(at.coupling[0])).T)

        settle()
        swap.wait_received()
        swap.wait_sent()
        other = at.other
        tail = jnp.concatenate([at.to_other[...], other[order:]], axis=0)
        _, _, sums = eliminate(count, blocks_of(other), chunks(tail), [((0, both), (0, order))])
        own_v[...] = own_v[...] - sums[0]
        scaled, lower, _ = eliminate(count, blocks_of(own_v), chunks(own_v[order:]), [])
        value_v[...] = resolve(scaled, lower)

    for level in range(levels - 1, -1, -1):
        distance = 2**level
        wide = level < levels - 1
        sends = lax.rem(place, 2 * distance) == 2 * distance - 1
        takes = lax.rem(place, 2 * distance) == distance - 1
        device = {"slab": jnp.where(takes, slab + inward * distance, slab - inward * distance)}
        back = remote(
            at.outbox[level], at.inbox[level],
            at.back.at[level, 0], at.back.at[level, 1], device,
        )

        @pl.when(sends)
        def _(level=level, wide=wide, back=back):
            kept, box = at.level_kept[level], at.outbox[level]
            found = kept[order:both] - dot(value_v[...], embed(kept[:order]))
            if wide:
                found = found - dot(value_u[...], embed(kept[both:]))
            box[rhs:] = value_u[...]
            box[:rhs] = found
            back.start()
            value_u[...] = found

        @pl.when(takes)
        def _(level=level, back=back):
            back.wait_recv()
            value_v[...] = at.inbox[level][:rhs]
            value_u[...] = at.inbox[level][rhs:]

        finish.append((sends, back.wait_send))

    kept = at.kept
    found = (
        kept[order:both]
        - dot(value_v[...], embed(kept[:order]))
        - dot(value_u[...], embed(kept[both:]))
    )
    result[at_interior] = separate(reversed_where(turned, found))
    result[1 - at_interior] = separate(value_v[...])
    for copy in sent:
        copy.wait_send()
    pl.when(shifts)(shift.wait_send)
    for condition, run in finish:
        pl.when(condition)(run)


def local(diag_blocks, couplings, sources):
    order, width = couplings.shape[1:]
    shard, rhs = diag_blocks.shape[1], sources.shape[1]
    count = order // HALF
    slabs, orbs = lax.axis_size("slab"), lax.axis_size("orb")
    levels = (slabs // 2).bit_length() - 1
    both = order + rhs
    square, tall, thin, lower = (
        (order, width), (both, width), (rhs, width), (count * (count - 1) // 2 * HALF, LANES),
    )
    dma = pltpu.SemaphoreType.DMA
    wide = (both + order, width)

    def vmem(*shape):
        return pltpu.VMEM(shape, jnp.float32)

    scratch = dict(
        diag=vmem(2, shard, width), load=vmem(2, rhs, width), coupling=vmem(2, order, width),
        interior=vmem(*square), boundary=vmem(*square), shifted=vmem(*square), pivot=vmem(*square),
        to_v=vmem(*square), outer=vmem(*square), kept=vmem(*wide), lower=vmem(*lower),
        inverse=vmem(count, LANES, LANES), across=vmem(count, LANES, (count - 1) * LANES),
        own_v=vmem(*tall), own_u=vmem(*tall), cross=vmem(*square), other=vmem(*tall),
        to_other=vmem(*square), value_v=vmem(*thin), value_u=vmem(*thin),
        fetch=dma((3,)), shift=dma((2,)), back=dma((max(1, levels), 2)),
        orb_send=dma((3, max(1, orbs - 1))), orb_receive=dma((3, max(1, orbs - 1))),
        relay=[relay_semaphores(count) for _ in range(levels + 1)],
        first_v=[vmem(*tall) for _ in range(levels)],
        level_kept=[vmem(*wide) if level < levels - 1 else vmem(*tall) for level in range(levels)],
        level_lower=[vmem(*lower) for _ in range(levels)],
        outbox=[vmem(2 * rhs, width) for _ in range(levels)],
        inbox=[vmem(2 * rhs, width) for _ in range(levels)],
        first_u=[vmem(*tall) for _ in range(levels - 1)],
        first_cross=[vmem(*square) for _ in range(levels - 1)],
        extra_send=[dma((2,)) for _ in range(levels - 1)],
        extra_receive=[dma((2,)) for _ in range(levels - 1)],
    )
    leaves, tree = jax.tree.flatten(scratch)
    return pl.pallas_call(
        functools.partial(solve_kernel, tree),
        out_shape=jax.ShapeDtypeStruct(sources.shape, jnp.float32),
        in_specs=[pl.BlockSpec(memory_space=pl.ANY)] * 3,
        out_specs=pl.BlockSpec(memory_space=pltpu.VMEM),
        scratch_shapes=leaves,
        compiler_params=pltpu.CompilerParams(
            vmem_limit_bytes=67043328, collective_id=0, has_side_effects=True
        ),
    )(diag_blocks, couplings, sources)


def solution(mesh):
    placed = (
        P(("energy", "slab"), "orb", None),
        P(("energy", "slab"), None, None),
        P(("energy", "slab"), ("orb", "rhs"), None),
    )
    return jax.shard_map(
        local,
        mesh=mesh,
        in_specs=placed,
        out_specs=P(("energy", "slab"), ("orb", "rhs"), None),
        check_vma=False,
    )
```

```python
import functools
import types

import jax
import jax.numpy as jnp
from jax import lax
from jax.sharding import PartitionSpec as P
from jax.experimental import pallas as pl
from jax.experimental.pallas import tpu as pltpu

HALF = 64
LANES = 2 * HALF


def dot(left, right, dims=((1,), (0,))):
    return lax.dot_general(
        left,
        right,
        (dims, ((), ())),
        precision=lax.Precision.HIGHEST,
        preferred_element_type=jnp.float32,
    )


def dot_flipped(left, right):
    return dot(left, right, ((1,), (1,)))


def lane_sign(shape):
    lane = lax.broadcasted_iota(jnp.int32, shape, 1)
    return jnp.where(lane % LANES < HALF, -1.0, 1.0).astype(jnp.float32)


def times_i(rows):
    pieces = [
        pltpu.roll(rows[:, start : start + LANES], HALF, 1)
        for start in range(0, rows.shape[1], LANES)
    ]
    turned = pieces[0] if len(pieces) == 1 else jnp.concatenate(pieces, axis=1)
    return turned * lane_sign(turned.shape)


def interleave(rows):
    count = rows.shape[1] // LANES
    pieces = []
    for chunk in range(count):
        pieces.append(rows[:, chunk * HALF : (chunk + 1) * HALF])
        pieces.append(rows[:, (count + chunk) * HALF : (count + chunk + 1) * HALF])
    return jnp.concatenate(pieces, axis=1)


def separate(rows):
    count = rows.shape[1] // LANES
    pieces = [rows[:, 2 * chunk * HALF : (2 * chunk + 1) * HALF] for chunk in range(count)]
    pieces += [rows[:, (2 * chunk + 1) * HALF : (2 * chunk + 2) * HALF] for chunk in range(count)]
    return jnp.concatenate(pieces, axis=1)


def embed(rows):
    turned = times_i(rows)
    pieces = []
    for start in range(0, rows.shape[0], HALF):
        pieces += [rows[start : start + HALF], turned[start : start + HALF]]
    return jnp.concatenate(pieces, axis=0)


def compact(embedded):
    return jnp.concatenate(
        [embedded[start : start + HALF] for start in range(0, embedded.shape[0], LANES)], axis=0
    )


GROUP = 16
TALL = 8


def product(left, right):
    return (left[0] * right[0] - left[1] * right[1], left[0] * right[1] + left[1] * right[0])


def minus(left, right):
    return (left[0] - right[0], left[1] - right[1])


def squared(value):
    return value[0] * value[0] + value[1] * value[1]


def spread_lane(rows, at):
    return jnp.broadcast_to(rows[:, at : at + 1], (TALL, LANES))


def pick(rows, at):
    return jnp.broadcast_to(rows[at : at + 1], (TALL, LANES))


def total(terms):
    while len(terms) > 1:
        terms = [sum(terms[i : i + 2][1:], terms[i]) for i in range(0, len(terms), 2)]
    return terms[0]


def spread_columns(part, step, count):
    return [(spread_lane(part, step + at), spread_lane(part, step + at + HALF)) for at in range(count)]


def invert_home(panel, spun, work, row_id):
    work = [tuple(jnp.where(row_id >= 0, half, 0.0) for half in value) for value in work]
    diagonal = pick(work[0][0], 0)
    for p in range(TALL):
        here = row_id == p
        real, imag = work[p]
        factor = 1.0 / diagonal
        across = {j: (pick(real, j), pick(imag, j)) for j in range(p + 1, TALL)}
        if p + 1 < TALL:
            diagonal = pick(work[p + 1][0], p + 1) - squared(across[p + 1]) * factor
        real = jnp.where(here, real - 1.0, real)
        imag = jnp.where(here, 0.0, imag)
        for j in range(p + 1, TALL):
            value = (across[j][0] * factor, across[j][1] * -factor)
            work[j] = minus(work[j], product((real, imag), value))
        row, turn = pick(panel, p) * factor, pick(spun, p) * factor
        panel = panel - (real * row + imag * turn)
        spun = spun - (real * turn - imag * row)
    return panel, spun


def invert_group(rows, first, sign, lane, row_id):
    above, below = rows[:TALL], rows[TALL:]
    inside = (lane % HALF >= first) & (lane % HALF < first + TALL)
    after = (lane % HALF >= first + TALL) & (lane % HALF < first + GROUP)
    home = spread_columns(above, first, TALL)
    side = spread_columns(below, first, TALL)
    panel = jnp.where(inside, 0.0, above)
    spun = pltpu.roll(panel, HALF, 1) * sign + jnp.where(lane == first + row_id + HALF, 1.0, 0.0)
    panel = panel + jnp.where(lane == first + row_id, 1.0, 0.0)
    panel, spun = invert_home(panel, spun, home, row_id)
    below = jnp.where(inside, 0.0, below) - total(
        [side[p][0] * pick(panel, p) + side[p][1] * pick(spun, p) for p in range(TALL)]
    )
    step = first + TALL
    home = spread_columns(below, step, TALL)
    side = spread_columns(panel, step, TALL)
    lower = jnp.where(after, 0.0, below)
    turned = pltpu.roll(lower, HALF, 1) * sign + jnp.where(lane == step + row_id + HALF, 1.0, 0.0)
    lower = lower + jnp.where(lane == step + row_id, 1.0, 0.0)
    lower, turned = invert_home(lower, turned, home, row_id)
    rows = [(pick(lower, p), pick(turned, p)) for p in range(TALL)]
    panel = jnp.where(after, 0.0, panel) - total(
        [side[p][0] * rows[p][0] + side[p][1] * rows[p][1] for p in range(TALL)]
    )
    spun = jnp.where(after, 0.0, spun) - total(
        [side[p][0] * rows[p][1] - side[p][1] * rows[p][0] for p in range(TALL)]
    )
    return jnp.concatenate([panel, lower], axis=0), jnp.concatenate([spun, turned], axis=0)


def spread_out(done, spun, first):
    last = HALF - first - GROUP
    before = [jnp.zeros((first, LANES), jnp.float32)] if first else []
    after = [jnp.zeros((last, LANES), jnp.float32)] if last else []
    return jnp.concatenate(before + [done] + after + before + [spun] + after, axis=0)


def invert_small(block, fillers=()):
    lane = lax.broadcasted_iota(jnp.int32, (1, LANES), 1)
    row_id = lax.broadcasted_iota(jnp.int32, (TALL, 1), 0)
    sign = lane_sign((1, LANES))
    group = block[:GROUP]
    fillers = list(fillers)
    slots = HALF // GROUP
    for first in range(0, HALF, GROUP):
        done, spun = invert_group(group, first, sign, lane, row_id)
        inside = (lane % HALF >= first) & (lane % HALF < first + GROUP)
        following = first + GROUP
        if following < HALF:
            parts = []
            for start in range(following, following + GROUP, TALL):
                old = block[start : start + TALL]
                columns = spread_columns(old, first, GROUP)
                parts.append(
                    jnp.where(inside, 0.0, old)
                    - total(
                        [
                            columns[at][0] * pick(done, at) + columns[at][1] * pick(spun, at)
                            for at in range(GROUP)
                        ]
                    )
                )
            group = jnp.concatenate(parts, axis=0)
        rest = jnp.where(inside, 0.0, block) - dot(
            jnp.where(inside, block, 0.0), spread_out(done, spun, first)
        )
        above = [rest[:first]] if first else []
        below = [rest[following:]] if following < HALF else []
        block = jnp.concatenate(above + [done] + below, axis=0)
        share = -(-len(fillers) // slots)
        for filler in fillers[:share]:
            filler()
        fillers, slots = fillers[share:], slots - 1
    return block


def doubled(rows):
    return jnp.concatenate([rows, times_i(rows)], axis=0)


def hermitian(block):
    return doubled(block).T[:HALF]


def chunk(rows, at):
    return rows[:, at * LANES : (at + 1) * LANES]


def chunks(rows):
    return [chunk(rows, at) for at in range(rows.shape[1] // LANES)]


def added(total_so_far, term):
    return term if total_so_far is None else total_so_far + term


def eliminate(count, block, make_tails, toward, before=None, keep=None, after=None):
    tails = []
    scaled = [None] * count
    lower = {}
    changes = {}
    sums = [None] * len(toward)
    pending = []

    def bulk(k, inverse, across, heads):
        def row_below(i):
            def run():
                lower[i, k] = dot(heads[i], inverse)
                change = dot(lower[i, k], across[:, (i - k - 1) * LANES :])
                for c in range(i, count):
                    changes[i, c] = added(changes.get((i, c)), chunk(change, c - i))

            return run

        def scale():
            scaled[k] = dot(tails[k], inverse)

        def shift():
            change = dot(scaled[k], across)
            for c in range(k + 1, count):
                tails[c] = tails[c] - chunk(change, c - k - 1)

        def gather(at):
            def run():
                (first, last), (low, high) = toward[at]
                term = dot_flipped(scaled[k][first:last], embed(tails[k][low:high]))
                sums[at] = added(sums[at], term)

            return run

        work = [row_below(i) for i in range(k + 2, count)] + [scale]
        if k + 1 < count:
            work.append(shift)
        return work + [gather(at) for at in range(len(toward))]

    def current(i, c):
        return block(i, c) - changes[i, c] if (i, c) in changes else block(i, c)

    for k in range(count):
        if before is not None:
            before(k)
        if k == min(1, count - 1):
            tails.extend(make_tails())
        inverse = doubled(invert_small(current(k, k), pending))
        if after is not None:
            after(k)
        across, heads = None, {}
        if k + 1 < count:
            right = [current(k, c) for c in range(k + 1, count)]
            across = doubled(jnp.concatenate(right, axis=1))
            heads = {i: hermitian(right[i - k - 1]) for i in range(k + 1, count)}
        if k + 1 < count:
            lower[k + 1, k] = dot(heads[k + 1], inverse)
            change = dot(lower[k + 1, k], across)
            for c in range(k + 1, count):
                changes[k + 1, c] = added(changes.get((k + 1, c)), chunk(change, c - k - 1))
        if keep is not None:
            keep(k, inverse, across)
        pending = bulk(k, inverse, across, heads)
    for work in pending:
        work()
    stacked = [lower[i, k] for k in range(count) for i in range(k + 1, count)]
    return jnp.concatenate(scaled, axis=1), jnp.concatenate(stacked, axis=0), sums


def resolve(rows, lower):
    count = rows.shape[1] // LANES
    places = [(i, k) for k in range(count) for i in range(k + 1, count)]
    found = chunks(rows)
    for i in range(count - 1, 0, -1):
        for k in range(i):
            at = places.index((i, k)) * HALF
            found[k] = found[k] - dot(found[i], doubled(lower[at : at + HALF]))
    return jnp.concatenate(found, axis=1)


def blocks_of(*refs):
    def block(i, c):
        rows, lanes = slice(i * HALF, (i + 1) * HALF), slice(c * LANES, (c + 1) * LANES)
        value = refs[0][rows, lanes]
        for ref in refs[1:]:
            value = value + ref[rows, lanes]
        return value

    return block


def remote(source, target, send, receive, device):
    return pltpu.make_async_remote_copy(
        src_ref=source, dst_ref=target, send_sem=send, recv_sem=receive,
        device_id=device, device_id_type=pl.DeviceIdType.MESH,
    )


class Move:
    def __init__(self, source, target, device, order, sems):
        self.source, self.target, self.device = source, target, device
        self.send, self.receive = sems
        self.count = order // HALF
        self.loads_at = min(1, self.count - 1)
        self.load = pl.ds(order, source.shape[0] - order)

    def copy(self, at, rows, lanes):
        return remote(
            self.source.at[rows, lanes], self.target.at[rows, lanes],
            self.send.at[at], self.receive.at[at], self.device,
        )

    def own(self, i):
        return self.copy(2 * i, pl.ds(i * HALF, HALF), pl.ds(i * LANES, LANES))

    def right(self, i):
        size = (self.count - 1 - i) * LANES
        return self.copy(2 * i + 1, pl.ds(i * HALF, HALF), pl.ds((i + 1) * LANES, size))

    def tail(self):
        return self.copy(2 * self.count, self.load, pl.ds(0, self.source.shape[1]))

    def copies(self):
        found = []
        for i in range(self.count):
            found.append(self.own(i))
            if i == self.loads_at:
                found.append(self.tail())
            if i + 1 < self.count:
                found.append(self.right(i))
        return found

    def start(self):
        for copy in self.copies():
            copy.start()

    def wait_sent(self):
        for copy in self.copies():
            copy.wait_send()

    def before(self, k):
        self.own(k).wait_recv()
        if k == self.loads_at:
            self.tail().wait_recv()

    def after(self, k):
        if k + 1 < self.count:
            self.right(k).wait_recv()


def move_semaphores(count):
    return [pltpu.SemaphoreType.DMA((2 * count + 1,)) for _ in range(2)]


def flipped_where(flip, ref, rows):
    @pl.when(flip)
    def _():
        ref[...] = compact(embed(rows).T)

    @pl.when(jnp.logical_not(flip))
    def _():
        ref[...] = rows


def reversed_where(flip, rows):
    pieces = chunks(rows)
    return jnp.where(flip, jnp.concatenate(pieces[::-1], axis=1), rows)


def solve_kernel(tree, diag, couplings, sources, result, *refs):
    at = types.SimpleNamespace(**jax.tree.unflatten(tree, refs))
    order, width = couplings.shape[1:]
    shard, rhs = diag.shape[1], sources.shape[1]
    count = order // HALF
    both = order + rhs
    slabs, orbs = lax.axis_size("slab"), lax.axis_size("orb")
    half = slabs // 2
    levels = half.bit_length() - 1
    slab, orb = lax.axis_index("slab"), lax.axis_index("orb")
    left = slab < half
    place = jnp.where(left, slab, slabs - 1 - slab)
    middle = place == half - 1
    inward = jnp.where(left, 1, -1)
    at_interior = jnp.where(left, 0, 1)
    paired = orbs == 2 and 2 * shard == 3 * HALF and order == 2 * shard
    turned = orb == 1 if paired else jnp.bool_(False)

    fetches = [
        pltpu.make_async_copy(ref, held, at.fetch.at[i])
        for i, (ref, held) in enumerate(((diag, at.diag), (couplings, at.coupling)))
    ]
    for fetch in fetches:
        fetch.start()
    barrier = pltpu.get_barrier_semaphore()

    def greet(device):
        pl.semaphore_signal(barrier, inc=1, device_id=device, device_id_type=pl.DeviceIdType.MESH)

    peers = [lax.rem(orb + step, orbs) for step in range(1, orbs)]
    owners = [lax.rem(orb + orbs - step, orbs) for step in range(1, orbs)]
    for device in [{"orb": peer} for peer in peers]:
        greet(device)
    expected = len(peers)
    for distance in sorted({1, *(2**level for level in range(levels))}):
        for other in (slab - distance, slab + distance):
            inside = (other >= 0) & (other < slabs)
            expected = expected + jnp.where(inside, 1, 0)
            pl.when(inside)(lambda other=other: greet({"slab": other}))
    fetches[0].wait()
    pl.semaphore_wait(barrier, expected)

    def rows_from(owner, low, size):
        return pl.ds(pl.multiple_of(owner * shard + low, 8), size)

    extra = shard - HALF
    if paired:
        def spans(owner):
            first = owner == 0
            return [(jnp.where(first, HALF, 0), extra), (jnp.where(first, 0, extra), HALF)]
    else:
        def spans(owner):
            return [(0, shard)]

    def gather_copies(gathered, layer, owner, step, device, first_sem, parts):
        return [
            remote(
                at.diag.at[layer, pl.ds(pl.multiple_of(low, 8), size)],
                gathered.at[rows_from(owner, low, size)],
                at.orb_send.at[first_sem + piece, step],
                at.orb_receive.at[first_sem + piece, step],
                device,
            )
            for piece, (low, size) in enumerate(parts)
        ]

    pieces = len(spans(orb))
    sent = []
    for step, peer in enumerate(peers):
        sent += gather_copies(
            at.interior, at_interior, orb, step, {"orb": peer}, 0, spans(orb)
        )
    for step, peer in enumerate(peers):
        sent += gather_copies(
            at.boundary, 1 - at_interior, orb, step, {"orb": peer}, pieces, [(0, shard)]
        )
    for copy in sent:
        copy.start()

    def wait_interior(piece):
        for step, owner in enumerate(owners):
            low, size = spans(owner)[piece]
            gather_copies(
                at.interior, at_interior, owner, step, {"orb": owner}, 0, spans(owner)
            )[piece].wait_recv()
            rows = rows_from(owner, low, size)
            at.pivot[rows] = interleave(at.interior[rows])

    def wait_boundary():
        for step, owner in enumerate(owners):
            gather_copies(
                at.boundary, 1 - at_interior, owner, step, {"orb": owner}, pieces, [(0, shard)]
            )[0].wait_recv()
        at.boundary[rows_from(orb, 0, shard)] = at.diag[1 - at_interior]

    fetches[1].wait()
    shift = remote(
        at.coupling.at[0], at.shifted, at.shift.at[0], at.shift.at[1],
        {"slab": jnp.where(slab > 0, slab - 1, 1)},
    )
    shifts = slab >= half
    pl.when(shifts)(shift.start)

    def place_of(position):
        return jnp.where(turned, count - 1 - position, position)

    def pivot_block(i, c):
        rows = pl.ds(pl.multiple_of(place_of(i) * HALF, HALF), HALF)
        return at.pivot[rows, pl.ds(pl.multiple_of(place_of(c) * LANES, LANES), LANES)]

    at.pivot[rows_from(orb, 0, shard)] = interleave(at.diag[at_interior])
    flipped_where(left, at.to_v, interleave(at.coupling[1]))
    tail = jnp.concatenate([at.to_v[...], interleave(sources[at_interior])], axis=0)

    def before(k):
        if paired and k > 0:
            wait_interior(k - 1)
        elif not paired and k == 0:
            wait_interior(0)

    def keep(k, inverse, across):
        at.inverse[k] = inverse
        if across is not None:
            at.across[k, :, : across.shape[1]] = across

    scaled, lower, sums = eliminate(
        count, pivot_block, lambda: chunks(reversed_where(turned, tail)), [((0, both), (0, order))],
        before, keep,
    )
    at.kept[:both] = scaled
    at.lower[...] = lower
    wait_boundary()
    own_v, own_u, cross = at.own_v, at.own_u, at.cross
    own_v[:order] = interleave(at.boundary[...]) - sums[0][:order]
    own_v[order:] = interleave(sources[1 - at_interior]) - sums[0][order:]

    def moved(level, source, target, device):
        return Move(source, target, device, order, at.moves[level])

    def outward():
        outer = at.outer

        @pl.when(left)
        def _():
            outer[...] = interleave(at.coupling[0])

        @pl.when(jnp.logical_not(left))
        def _():
            shift.wait_recv()
            outer[...] = compact(embed(interleave(at.shifted[...])).T)

        tails = chunks(reversed_where(turned, outer[...]))
        total_u = None
        for k in range(count):
            found = dot(tails[k], at.inverse[k])
            if k + 1 < count:
                change = dot(found, at.across[k, :, : (count - 1 - k) * LANES])
                for c in range(k + 1, count):
                    tails[c] = tails[c] - chunk(change, c - k - 1)
            lanes = slice(k * LANES, (k + 1) * LANES)
            at.kept[both:, lanes] = found
            stacked = jnp.concatenate([at.kept[:both, lanes], found], axis=0)
            total_u = added(total_u, dot_flipped(stacked, embed(tails[k])))
        own_u[:order] = -total_u[both:]
        own_u[order:] = -total_u[order:both]
        cross[...] = -total_u[:order]

    def no_outward():
        own_u[...] = jnp.zeros(own_u.shape, jnp.float32)
        cross[...] = jnp.zeros(cross.shape, jnp.float32)
        at.kept[both:] = jnp.zeros((order, width), jnp.float32)

    def settle():
        at.kept[...] = resolve(at.kept[...], at.lower[...])

    def settle_levels(below):
        for level in range(below):
            kept = at.level_kept[level]
            kept[...] = resolve(kept[...], at.level_lower[level][...])

    finish = []
    for level in range(levels):
        distance = 2**level
        wide = level < levels - 1
        sends = lax.rem(place, 2 * distance) == distance - 1
        takes = lax.rem(place, 2 * distance) == 2 * distance - 1
        device = {"slab": jnp.where(sends, slab + inward * distance, slab - inward * distance)}
        first_v = at.first_v[level]
        move = moved(level, own_v, first_v, device)
        pl.when(sends)(move.start)
        if level == 0:
            pl.when(place > 0)(outward)
            pl.when(place == 0)(no_outward)
        extras = []
        if wide:
            extras = [
                remote(
                    ref, target,
                    at.extra_send[level].at[i], at.extra_receive[level].at[i], device,
                )
                for i, (ref, target) in enumerate(
                    ((own_u, at.first_u[level]), (cross, at.first_cross[level]))
                )
            ]
            for copy in extras:
                pl.when(sends)(copy.start)
        kept, level_lower = at.level_kept[level], at.level_lower[level]

        @pl.when(sends)
        def _(level=level):
            settle()
            settle_levels(level)

        @pl.when(takes)
        def _(level=level, wide=wide, move=move, extras=extras, first_v=first_v, kept=kept, level_lower=level_lower):
            toward = [((0, both), (0, order))]
            if wide:
                toward.append(((0, both + order), (both, both + order)))

            def tails():
                parts = [cross[...], first_v[order:] + own_u[order:]]
                for copy in extras:
                    copy.wait_recv()
                if wide:
                    parts.append(compact(embed(at.first_cross[level][...]).T))
                return chunks(jnp.concatenate(parts, axis=0))

            scaled, lower, sums = eliminate(
                count, blocks_of(first_v, own_u), tails, toward, before=move.before, after=move.after
            )
            kept[...] = scaled
            level_lower[...] = lower
            own_v[...] = own_v[...] - sums[0]
            if wide:
                first_u = at.first_u[level]
                own_u[:order] = first_u[:order] - sums[1][both:]
                own_u[order:] = first_u[order:] - sums[1][order:both]
                cross[...] = -sums[1][:order]

        def sent_all(move=move, extras=extras):
            move.wait_sent()
            for copy in extras:
                copy.wait_send()

        finish.append((sends, sent_all))

    value_v, value_u = at.value_v, at.value_u
    value_u[...] = jnp.zeros(value_u.shape, jnp.float32)
    swap = moved(levels, own_v, at.other, {"slab": jnp.where(left, half, half - 1)})

    @pl.when(middle)
    def _():
        swap.start()
        settle_levels(levels)

        @pl.when(left)
        def _():
            shift.wait_recv()
            at.to_other[...] = interleave(at.shifted[...])

        @pl.when(jnp.logical_not(left))
        def _():
            at.to_other[...] = compact(embed(interleave(at.coupling[0])).T)

        other = at.other

        def swapped(k):
            swap.before(k)
            if k == count - 1:
                swap.wait_sent()

        _, _, sums = eliminate(
            count, blocks_of(other),
            lambda: chunks(jnp.concatenate([at.to_other[...], other[order:]], axis=0)),
            [((0, both), (0, order))], before=swapped, after=swap.after,
        )
        reduced = own_v[...] - sums[0]
        scaled, lower, _ = eliminate(
            count, blocks_of(reduced), lambda: chunks(reduced[order:]), []
        )
        value_v[...] = resolve(scaled, lower)

    for level in range(levels - 1, -1, -1):
        distance = 2**level
        wide = level < levels - 1
        sends = lax.rem(place, 2 * distance) == 2 * distance - 1
        takes = lax.rem(place, 2 * distance) == distance - 1
        device = {"slab": jnp.where(takes, slab + inward * distance, slab - inward * distance)}
        back = remote(
            at.outbox[level], at.inbox[level],
            at.back.at[level, 0], at.back.at[level, 1], device,
        )

        @pl.when(sends)
        def _(level=level, wide=wide, back=back):
            kept, box = at.level_kept[level], at.outbox[level]
            found = kept[order:both] - dot(value_v[...], embed(kept[:order]))
            if wide:
                found = found - dot(value_u[...], embed(kept[both:]))
            box[rhs:] = value_u[...]
            box[:rhs] = found
            back.start()
            value_u[...] = found

        @pl.when(takes)
        def _(level=level, back=back):
            back.wait_recv()
            value_v[...] = at.inbox[level][:rhs]
            value_u[...] = at.inbox[level][rhs:]

        finish.append((sends, back.wait_send))

    kept = at.kept
    found = (
        kept[order:both]
        - dot(value_v[...], embed(kept[:order]))
        - dot(value_u[...], embed(kept[both:]))
    )

    @pl.when(middle)
    def _():
        result[at_interior] = separate(reversed_where(turned, resolve(found, at.lower[...])))

    @pl.when(jnp.logical_not(middle))
    def _():
        result[at_interior] = separate(reversed_where(turned, found))

    result[1 - at_interior] = separate(value_v[...])
    for copy in sent:
        copy.wait_send()
    pl.when(shifts)(shift.wait_send)
    for condition, run in finish:
        pl.when(condition)(run)


def local(diag_blocks, couplings, sources):
    order, width = couplings.shape[1:]
    shard, rhs = diag_blocks.shape[1], sources.shape[1]
    count = order // HALF
    slabs, orbs = lax.axis_size("slab"), lax.axis_size("orb")
    levels = (slabs // 2).bit_length() - 1
    both = order + rhs
    square, tall, thin, lower = (
        (order, width), (both, width), (rhs, width), (count * (count - 1) // 2 * HALF, LANES),
    )
    dma = pltpu.SemaphoreType.DMA
    wide = (both + order, width)

    def vmem(*shape):
        return pltpu.VMEM(shape, jnp.float32)

    scratch = dict(
        diag=vmem(2, shard, width), coupling=vmem(2, order, width),
        interior=vmem(*square), boundary=vmem(*square), shifted=vmem(*square), pivot=vmem(*square),
        to_v=vmem(*square), outer=vmem(*square), kept=vmem(*wide), lower=vmem(*lower),
        inverse=vmem(count, LANES, LANES), across=vmem(count, LANES, (count - 1) * LANES),
        own_v=vmem(*tall), own_u=vmem(*tall), cross=vmem(*square), other=vmem(*tall),
        to_other=vmem(*square), value_v=vmem(*thin), value_u=vmem(*thin),
        fetch=dma((2,)), shift=dma((2,)), back=dma((max(1, levels), 2)),
        orb_send=dma((3, max(1, orbs - 1))), orb_receive=dma((3, max(1, orbs - 1))),
        moves=[move_semaphores(count) for _ in range(levels + 1)],
        first_v=[vmem(*tall) for _ in range(levels)],
        level_kept=[vmem(*wide) if level < levels - 1 else vmem(*tall) for level in range(levels)],
        level_lower=[vmem(*lower) for _ in range(levels)],
        outbox=[vmem(2 * rhs, width) for _ in range(levels)],
        inbox=[vmem(2 * rhs, width) for _ in range(levels)],
        first_u=[vmem(*tall) for _ in range(levels - 1)],
        first_cross=[vmem(*square) for _ in range(levels - 1)],
        extra_send=[dma((2,)) for _ in range(levels - 1)],
        extra_receive=[dma((2,)) for _ in range(levels - 1)],
    )
    leaves, tree = jax.tree.flatten(scratch)
    return pl.pallas_call(
        functools.partial(solve_kernel, tree),
        out_shape=jax.ShapeDtypeStruct(sources.shape, jnp.float32),
        in_specs=[pl.BlockSpec(memory_space=space) for space in (pl.ANY, pl.ANY, pltpu.VMEM)],
        out_specs=pl.BlockSpec(memory_space=pltpu.VMEM),
        scratch_shapes=leaves,
        compiler_params=pltpu.CompilerParams(
            vmem_limit_bytes=67043328 - 131072, collective_id=0, has_side_effects=True
        ),
    )(diag_blocks, couplings, sources)


def solution(mesh):
    placed = (
        P(("energy", "slab"), "orb", None),
        P(("energy", "slab"), None, None),
        P(("energy", "slab"), ("orb", "rhs"), None),
    )
    return jax.shard_map(
        local,
        mesh=mesh,
        in_specs=placed,
        out_specs=P(("energy", "slab"), ("orb", "rhs"), None),
        check_vma=False,
    )
```

```python
import functools
import types

import jax
import jax.numpy as jnp
from jax import lax
from jax.sharding import PartitionSpec as P
from jax.experimental import pallas as pl
from jax.experimental.pallas import tpu as pltpu

HALF = 64
LANES = 2 * HALF


def dot(left, right, dims=((1,), (0,))):
    return lax.dot_general(
        left,
        right,
        (dims, ((), ())),
        precision=lax.Precision.HIGHEST,
        preferred_element_type=jnp.float32,
    )


def dot_flipped(left, right):
    return dot(left, right, ((1,), (1,)))


def lane_sign(shape):
    lane = lax.broadcasted_iota(jnp.int32, shape, 1)
    return jnp.where(lane % LANES < HALF, -1.0, 1.0).astype(jnp.float32)


def times_i(rows):
    pieces = [
        pltpu.roll(rows[:, start : start + LANES], HALF, 1)
        for start in range(0, rows.shape[1], LANES)
    ]
    turned = pieces[0] if len(pieces) == 1 else jnp.concatenate(pieces, axis=1)
    return turned * lane_sign(turned.shape)


def interleave(rows):
    count = rows.shape[1] // LANES
    pieces = []
    for chunk in range(count):
        pieces.append(rows[:, chunk * HALF : (chunk + 1) * HALF])
        pieces.append(rows[:, (count + chunk) * HALF : (count + chunk + 1) * HALF])
    return jnp.concatenate(pieces, axis=1)


def separate(rows):
    count = rows.shape[1] // LANES
    pieces = [rows[:, 2 * chunk * HALF : (2 * chunk + 1) * HALF] for chunk in range(count)]
    pieces += [rows[:, (2 * chunk + 1) * HALF : (2 * chunk + 2) * HALF] for chunk in range(count)]
    return jnp.concatenate(pieces, axis=1)


def embed(rows):
    turned = times_i(rows)
    pieces = []
    for start in range(0, rows.shape[0], HALF):
        pieces += [rows[start : start + HALF], turned[start : start + HALF]]
    return jnp.concatenate(pieces, axis=0)


def compact(embedded):
    return jnp.concatenate(
        [embedded[start : start + HALF] for start in range(0, embedded.shape[0], LANES)], axis=0
    )


GROUP = 16
TALL = 8


def product(left, right):
    return (left[0] * right[0] - left[1] * right[1], left[0] * right[1] + left[1] * right[0])


def minus(left, right):
    return (left[0] - right[0], left[1] - right[1])


def squared(value):
    return value[0] * value[0] + value[1] * value[1]


def spread_lane(rows, at):
    return jnp.broadcast_to(rows[:, at : at + 1], (TALL, LANES))


def pick(rows, at):
    return jnp.broadcast_to(rows[at : at + 1], (TALL, LANES))


def total(terms):
    while len(terms) > 1:
        terms = [sum(terms[i : i + 2][1:], terms[i]) for i in range(0, len(terms), 2)]
    return terms[0]


def spread_columns(part, step, count):
    return [(spread_lane(part, step + at), spread_lane(part, step + at + HALF)) for at in range(count)]


def invert_home(panel, spun, work, row_id):
    work = [tuple(jnp.where(row_id >= 0, half, 0.0) for half in value) for value in work]
    diagonal = pick(work[0][0], 0)
    for p in range(TALL):
        here = row_id == p
        real, imag = work[p]
        factor = 1.0 / diagonal
        across = {j: (pick(real, j), pick(imag, j)) for j in range(p + 1, TALL)}
        if p + 1 < TALL:
            diagonal = pick(work[p + 1][0], p + 1) - squared(across[p + 1]) * factor
        real = jnp.where(here, real - 1.0, real)
        imag = jnp.where(here, 0.0, imag)
        for j in range(p + 1, TALL):
            value = (across[j][0] * factor, across[j][1] * -factor)
            work[j] = minus(work[j], product((real, imag), value))
        row, turn = pick(panel, p) * factor, pick(spun, p) * factor
        panel = panel - (real * row + imag * turn)
        spun = spun - (real * turn - imag * row)
    return panel, spun


def invert_group(rows, first, sign, lane, row_id):
    above, below = rows[:TALL], rows[TALL:]
    inside = (lane % HALF >= first) & (lane % HALF < first + TALL)
    after = (lane % HALF >= first + TALL) & (lane % HALF < first + GROUP)
    home = spread_columns(above, first, TALL)
    side = spread_columns(below, first, TALL)
    panel = jnp.where(inside, 0.0, above)
    spun = pltpu.roll(panel, HALF, 1) * sign + jnp.where(lane == first + row_id + HALF, 1.0, 0.0)
    panel = panel + jnp.where(lane == first + row_id, 1.0, 0.0)
    panel, spun = invert_home(panel, spun, home, row_id)
    below = jnp.where(inside, 0.0, below) - total(
        [side[p][0] * pick(panel, p) + side[p][1] * pick(spun, p) for p in range(TALL)]
    )
    step = first + TALL
    home = spread_columns(below, step, TALL)
    side = spread_columns(panel, step, TALL)
    lower = jnp.where(after, 0.0, below)
    turned = pltpu.roll(lower, HALF, 1) * sign + jnp.where(lane == step + row_id + HALF, 1.0, 0.0)
    lower = lower + jnp.where(lane == step + row_id, 1.0, 0.0)
    lower, turned = invert_home(lower, turned, home, row_id)
    rows = [(pick(lower, p), pick(turned, p)) for p in range(TALL)]
    panel = jnp.where(after, 0.0, panel) - total(
        [side[p][0] * rows[p][0] + side[p][1] * rows[p][1] for p in range(TALL)]
    )
    spun = jnp.where(after, 0.0, spun) - total(
        [side[p][0] * rows[p][1] - side[p][1] * rows[p][0] for p in range(TALL)]
    )
    return jnp.concatenate([panel, lower], axis=0), jnp.concatenate([spun, turned], axis=0)


def spread_out(done, spun, first):
    last = HALF - first - GROUP
    before = [jnp.zeros((first, LANES), jnp.float32)] if first else []
    after = [jnp.zeros((last, LANES), jnp.float32)] if last else []
    return jnp.concatenate(before + [done] + after + before + [spun] + after, axis=0)


def invert_small(block, fillers=()):
    lane = lax.broadcasted_iota(jnp.int32, (1, LANES), 1)
    row_id = lax.broadcasted_iota(jnp.int32, (TALL, 1), 0)
    sign = lane_sign((1, LANES))
    group = block[:GROUP]
    fillers = list(fillers)
    slots = HALF // GROUP
    for first in range(0, HALF, GROUP):
        done, spun = invert_group(group, first, sign, lane, row_id)
        inside = (lane % HALF >= first) & (lane % HALF < first + GROUP)
        following = first + GROUP
        if following < HALF:
            parts = []
            for start in range(following, following + GROUP, TALL):
                old = block[start : start + TALL]
                columns = spread_columns(old, first, GROUP)
                parts.append(
                    jnp.where(inside, 0.0, old)
                    - total(
                        [
                            columns[at][0] * pick(done, at) + columns[at][1] * pick(spun, at)
                            for at in range(GROUP)
                        ]
                    )
                )
            group = jnp.concatenate(parts, axis=0)
        rest = jnp.where(inside, 0.0, block) - dot(
            jnp.where(inside, block, 0.0), spread_out(done, spun, first)
        )
        above = [rest[:first]] if first else []
        below = [rest[following:]] if following < HALF else []
        block = jnp.concatenate(above + [done] + below, axis=0)
        share = -(-len(fillers) // slots)
        for filler in fillers[:share]:
            filler()
        fillers, slots = fillers[share:], slots - 1
    return block


def doubled(rows):
    return jnp.concatenate([rows, times_i(rows)], axis=0)


def hermitian(block):
    return doubled(block).T[:HALF]


def chunk(rows, at):
    return rows[:, at * LANES : (at + 1) * LANES]


def chunks(rows):
    return [chunk(rows, at) for at in range(rows.shape[1] // LANES)]


def added(total_so_far, term):
    return term if total_so_far is None else total_so_far + term


def eliminate(count, block, make_tails, toward, before=None, keep=None, after=None):
    tails = []
    scaled = [None] * count
    lower = {}
    changes = {}
    sums = [None] * len(toward)
    pending = []

    def bulk(k, inverse, across, heads):
        def row_below(i):
            def run():
                lower[i, k] = dot(heads[i], inverse)
                change = dot(lower[i, k], across[:, (i - k - 1) * LANES :])
                for c in range(i, count):
                    changes[i, c] = added(changes.get((i, c)), chunk(change, c - i))

            return run

        def scale():
            scaled[k] = dot(tails[k], inverse)

        def shift():
            change = dot(scaled[k], across)
            for c in range(k + 1, count):
                tails[c] = tails[c] - chunk(change, c - k - 1)

        def gather(at):
            def run():
                (first, last), (low, high) = toward[at]
                term = dot_flipped(scaled[k][first:last], embed(tails[k][low:high]))
                sums[at] = added(sums[at], term)

            return run

        work = [row_below(i) for i in range(k + 2, count)] + [scale]
        if k + 1 < count:
            work.append(shift)
        return work + [gather(at) for at in range(len(toward))]

    def current(i, c):
        return block(i, c) - changes[i, c] if (i, c) in changes else block(i, c)

    for k in range(count):
        if before is not None:
            before(k)
        if k == min(1, count - 1):
            tails.extend(make_tails())
        inverse = doubled(invert_small(current(k, k), pending))
        if after is not None:
            after(k)
        across, heads = None, {}
        if k + 1 < count:
            right = [current(k, c) for c in range(k + 1, count)]
            across = doubled(jnp.concatenate(right, axis=1))
            heads = {i: hermitian(right[i - k - 1]) for i in range(k + 1, count)}
        if k + 1 < count:
            lower[k + 1, k] = dot(heads[k + 1], inverse)
            change = dot(lower[k + 1, k], across)
            for c in range(k + 1, count):
                changes[k + 1, c] = added(changes.get((k + 1, c)), chunk(change, c - k - 1))
        if keep is not None:
            keep(k, inverse, across)
        pending = bulk(k, inverse, across, heads)
    for work in pending:
        work()
    stacked = [lower[i, k] for k in range(count) for i in range(k + 1, count)]
    return jnp.concatenate(scaled, axis=1), jnp.concatenate(stacked, axis=0), sums


def resolve(rows, lower):
    count = rows.shape[1] // LANES
    places = [(i, k) for k in range(count) for i in range(k + 1, count)]
    found = chunks(rows)
    for i in range(count - 1, 0, -1):
        for k in range(i):
            at = places.index((i, k)) * HALF
            found[k] = found[k] - dot(found[i], doubled(lower[at : at + HALF]))
    return jnp.concatenate(found, axis=1)


def blocks_of(*refs):
    def block(i, c):
        rows, lanes = slice(i * HALF, (i + 1) * HALF), slice(c * LANES, (c + 1) * LANES)
        value = refs[0][rows, lanes]
        for ref in refs[1:]:
            value = value + ref[rows, lanes]
        return value

    return block


def remote(source, target, send, receive, device):
    return pltpu.make_async_remote_copy(
        src_ref=source, dst_ref=target, send_sem=send, recv_sem=receive,
        device_id=device, device_id_type=pl.DeviceIdType.MESH,
    )


class Move:
    def __init__(self, source, target, device, order, sems):
        self.source, self.target, self.device = source, target, device
        self.send, self.receive = sems
        self.count = order // HALF
        self.loads_at = min(1, self.count - 1)
        self.load = pl.ds(order, source.shape[0] - order)

    def copy(self, at, rows, lanes):
        return remote(
            self.source.at[rows, lanes], self.target.at[rows, lanes],
            self.send.at[at], self.receive.at[at], self.device,
        )

    def own(self, i):
        return self.copy(2 * i, pl.ds(i * HALF, HALF), pl.ds(i * LANES, LANES))

    def right(self, i):
        size = (self.count - 1 - i) * LANES
        return self.copy(2 * i + 1, pl.ds(i * HALF, HALF), pl.ds((i + 1) * LANES, size))

    def tail(self):
        return self.copy(2 * self.count, self.load, pl.ds(0, self.source.shape[1]))

    def copies(self):
        found = []
        for i in range(self.count):
            found.append(self.own(i))
            if i == self.loads_at:
                found.append(self.tail())
            if i + 1 < self.count:
                found.append(self.right(i))
        return found

    def start(self):
        for copy in self.copies():
            copy.start()

    def wait_sent(self):
        for copy in self.copies():
            copy.wait_send()

    def before(self, k):
        self.own(k).wait_recv()
        if k == self.loads_at:
            self.tail().wait_recv()

    def after(self, k):
        if k + 1 < self.count:
            self.right(k).wait_recv()


def move_semaphores(count):
    return [pltpu.SemaphoreType.DMA((2 * count + 1,)) for _ in range(2)]


def flipped_where(flip, ref, rows):
    @pl.when(flip)
    def _():
        ref[...] = compact(embed(rows).T)

    @pl.when(jnp.logical_not(flip))
    def _():
        ref[...] = rows


def reversed_where(flip, rows):
    pieces = chunks(rows)
    return jnp.where(flip, jnp.concatenate(pieces[::-1], axis=1), rows)


def solve_kernel(tree, diag, couplings, sources, result, *refs):
    at = types.SimpleNamespace(**jax.tree.unflatten(tree, refs))
    order, width = couplings.shape[1:]
    shard, rhs = diag.shape[1], sources.shape[1]
    count = order // HALF
    both = order + rhs
    slabs, orbs = lax.axis_size("slab"), lax.axis_size("orb")
    half = slabs // 2
    levels = half.bit_length() - 1
    slab, orb = lax.axis_index("slab"), lax.axis_index("orb")
    left = slab < half
    place = jnp.where(left, slab, slabs - 1 - slab)
    middle = place == half - 1
    inward = jnp.where(left, 1, -1)
    at_interior = jnp.where(left, 0, 1)
    paired = orbs == 2 and 2 * shard == 3 * HALF and order == 2 * shard
    turned = orb == 1 if paired else jnp.bool_(False)

    fetches = [
        pltpu.make_async_copy(ref, held, at.fetch.at[i])
        for i, (ref, held) in enumerate(((diag, at.diag), (couplings, at.coupling), (sources, at.load)))
    ]
    for fetch in fetches:
        fetch.start()
    barrier = pltpu.get_barrier_semaphore()

    def greet(device):
        pl.semaphore_signal(barrier, inc=1, device_id=device, device_id_type=pl.DeviceIdType.MESH)

    peers = [lax.rem(orb + step, orbs) for step in range(1, orbs)]
    owners = [lax.rem(orb + orbs - step, orbs) for step in range(1, orbs)]
    for device in [{"orb": peer} for peer in peers]:
        greet(device)
    expected = len(peers)
    for distance in sorted({1, *(2**level for level in range(levels))}):
        for other in (slab - distance, slab + distance):
            inside = (other >= 0) & (other < slabs)
            expected = expected + jnp.where(inside, 1, 0)
            pl.when(inside)(lambda other=other: greet({"slab": other}))
    fetches[0].wait()
    pl.semaphore_wait(barrier, expected)

    def rows_from(owner, low, size):
        return pl.ds(pl.multiple_of(owner * shard + low, 8), size)

    extra = shard - HALF
    if paired:
        def spans(owner):
            first = owner == 0
            return [(jnp.where(first, HALF, 0), extra), (jnp.where(first, 0, extra), HALF)]
    else:
        def spans(owner):
            return [(0, shard)]

    def gather_copies(gathered, layer, owner, step, device, first_sem, parts):
        return [
            remote(
                at.diag.at[layer, pl.ds(pl.multiple_of(low, 8), size)],
                gathered.at[rows_from(owner, low, size)],
                at.orb_send.at[first_sem + piece, step],
                at.orb_receive.at[first_sem + piece, step],
                device,
            )
            for piece, (low, size) in enumerate(parts)
        ]

    pieces = len(spans(orb))
    sent = []
    for step, peer in enumerate(peers):
        sent += gather_copies(
            at.interior, at_interior, orb, step, {"orb": peer}, 0, spans(orb)
        )
    for step, peer in enumerate(peers):
        sent += gather_copies(
            at.boundary, 1 - at_interior, orb, step, {"orb": peer}, pieces, [(0, shard)]
        )
    for copy in sent:
        copy.start()

    def wait_interior(piece):
        for step, owner in enumerate(owners):
            low, size = spans(owner)[piece]
            gather_copies(
                at.interior, at_interior, owner, step, {"orb": owner}, 0, spans(owner)
            )[piece].wait_recv()
            rows = rows_from(owner, low, size)
            at.pivot[rows] = interleave(at.interior[rows])

    def wait_boundary():
        for step, owner in enumerate(owners):
            gather_copies(
                at.boundary, 1 - at_interior, owner, step, {"orb": owner}, pieces, [(0, shard)]
            )[0].wait_recv()
        at.boundary[rows_from(orb, 0, shard)] = at.diag[1 - at_interior]

    fetches[1].wait()
    fetches[2].wait()
    shift = remote(
        at.coupling.at[0], at.shifted, at.shift.at[0], at.shift.at[1],
        {"slab": jnp.where(slab > 0, slab - 1, 1)},
    )
    shifts = slab >= half
    pl.when(shifts)(shift.start)

    def place_of(position):
        return jnp.where(turned, count - 1 - position, position)

    def pivot_block(i, c):
        rows = pl.ds(pl.multiple_of(place_of(i) * HALF, HALF), HALF)
        return at.pivot[rows, pl.ds(pl.multiple_of(place_of(c) * LANES, LANES), LANES)]

    at.pivot[rows_from(orb, 0, shard)] = interleave(at.diag[at_interior])

    def before(k):
        if k == min(1, count - 1):
            flipped_where(left, at.to_v, interleave(at.coupling[1]))
        if paired and k > 0:
            wait_interior(k - 1)
        elif not paired and k == 0:
            wait_interior(0)

    def interior_tails():
        tail = jnp.concatenate([at.to_v[...], interleave(at.load[at_interior])], axis=0)
        return chunks(reversed_where(turned, tail))

    def keep(k, inverse, across):
        at.inverse[k] = inverse
        if across is not None:
            at.across[k, :, : across.shape[1]] = across

    scaled, lower, sums = eliminate(
        count, pivot_block, interior_tails, [((0, both), (0, order))],
        before, keep,
    )
    at.kept[:both] = scaled
    at.lower[...] = lower
    wait_boundary()
    own_v, own_u, cross = at.own_v, at.own_u, at.cross
    own_v[:order] = interleave(at.boundary[...]) - sums[0][:order]
    own_v[order:] = interleave(at.load[1 - at_interior]) - sums[0][order:]

    def moved(level, source, target, device):
        return Move(source, target, device, order, at.moves[level])

    def outward():
        outer = at.outer

        @pl.when(left)
        def _():
            outer[...] = interleave(at.coupling[0])

        @pl.when(jnp.logical_not(left))
        def _():
            shift.wait_recv()
            outer[...] = compact(embed(interleave(at.shifted[...])).T)

        tails = chunks(reversed_where(turned, outer[...]))
        total_u = None
        for k in range(count):
            found = dot(tails[k], at.inverse[k])
            if k + 1 < count:
                change = dot(found, at.across[k, :, : (count - 1 - k) * LANES])
                for c in range(k + 1, count):
                    tails[c] = tails[c] - chunk(change, c - k - 1)
            lanes = slice(k * LANES, (k + 1) * LANES)
            at.kept[both:, lanes] = found
            stacked = jnp.concatenate([at.kept[:both, lanes], found], axis=0)
            total_u = added(total_u, dot_flipped(stacked, embed(tails[k])))
        own_u[:order] = -total_u[both:]
        own_u[order:] = -total_u[order:both]
        cross[...] = -total_u[:order]

    def no_outward():
        own_u[...] = jnp.zeros(own_u.shape, jnp.float32)
        cross[...] = jnp.zeros(cross.shape, jnp.float32)
        at.kept[both:] = jnp.zeros((order, width), jnp.float32)

    def settle():
        at.kept[...] = resolve(at.kept[...], at.lower[...])

    def settle_levels(below):
        for level in range(below):
            kept = at.level_kept[level]
            kept[...] = resolve(kept[...], at.level_lower[level][...])

    finish = []
    for level in range(levels):
        distance = 2**level
        wide = level < levels - 1
        sends = lax.rem(place, 2 * distance) == distance - 1
        takes = lax.rem(place, 2 * distance) == 2 * distance - 1
        device = {"slab": jnp.where(sends, slab + inward * distance, slab - inward * distance)}
        first_v = at.first_v[level]
        move = moved(level, own_v, first_v, device)
        pl.when(sends)(move.start)
        if level == 0:
            pl.when(place > 0)(outward)
            pl.when(place == 0)(no_outward)
        extras = []
        if wide:
            extras = [
                remote(
                    ref, target,
                    at.extra_send[level].at[i], at.extra_receive[level].at[i], device,
                )
                for i, (ref, target) in enumerate(
                    ((own_u, at.first_u[level]), (cross, at.first_cross[level]))
                )
            ]
            for copy in extras:
                pl.when(sends)(copy.start)
        kept, level_lower = at.level_kept[level], at.level_lower[level]

        @pl.when(sends)
        def _(level=level):
            settle()
            settle_levels(level)

        @pl.when(takes)
        def _(level=level, wide=wide, move=move, extras=extras, first_v=first_v, kept=kept, level_lower=level_lower):
            toward = [((0, both), (0, order))]
            if wide:
                toward.append(((0, both + order), (both, both + order)))

            def tails():
                parts = [cross[...], first_v[order:] + own_u[order:]]
                for copy in extras:
                    copy.wait_recv()
                if wide:
                    parts.append(compact(embed(at.first_cross[level][...]).T))
                return chunks(jnp.concatenate(parts, axis=0))

            scaled, lower, sums = eliminate(
                count, blocks_of(first_v, own_u), tails, toward, before=move.before, after=move.after
            )
            kept[...] = scaled
            level_lower[...] = lower
            own_v[...] = own_v[...] - sums[0]
            if wide:
                first_u = at.first_u[level]
                own_u[:order] = first_u[:order] - sums[1][both:]
                own_u[order:] = first_u[order:] - sums[1][order:both]
                cross[...] = -sums[1][:order]

        def sent_all(move=move, extras=extras):
            move.wait_sent()
            for copy in extras:
                copy.wait_send()

        finish.append((sends, sent_all))

    value_v, value_u = at.value_v, at.value_u
    value_u[...] = jnp.zeros(value_u.shape, jnp.float32)
    swap = moved(levels, own_v, at.other, {"slab": jnp.where(left, half, half - 1)})

    @pl.when(middle)
    def _():
        swap.start()
        settle_levels(levels)

        @pl.when(left)
        def _():
            shift.wait_recv()
            at.to_other[...] = interleave(at.shifted[...])

        @pl.when(jnp.logical_not(left))
        def _():
            at.to_other[...] = compact(embed(interleave(at.coupling[0])).T)

        other = at.other

        def swapped(k):
            swap.before(k)
            if k == count - 1:
                swap.wait_sent()

        _, _, sums = eliminate(
            count, blocks_of(other),
            lambda: chunks(jnp.concatenate([at.to_other[...], other[order:]], axis=0)),
            [((0, both), (0, order))], before=swapped, after=swap.after,
        )
        reduced = own_v[...] - sums[0]
        scaled, lower, _ = eliminate(
            count, blocks_of(reduced), lambda: chunks(reduced[order:]), []
        )
        value_v[...] = resolve(scaled, lower)

    for level in range(levels - 1, -1, -1):
        distance = 2**level
        wide = level < levels - 1
        sends = lax.rem(place, 2 * distance) == 2 * distance - 1
        takes = lax.rem(place, 2 * distance) == distance - 1
        device = {"slab": jnp.where(takes, slab + inward * distance, slab - inward * distance)}
        back = remote(
            at.outbox[level], at.inbox[level],
            at.back.at[level, 0], at.back.at[level, 1], device,
        )

        @pl.when(sends)
        def _(level=level, wide=wide, back=back):
            kept, box = at.level_kept[level], at.outbox[level]
            found = kept[order:both] - dot(value_v[...], embed(kept[:order]))
            if wide:
                found = found - dot(value_u[...], embed(kept[both:]))
            box[rhs:] = value_u[...]
            box[:rhs] = found
            back.start()
            value_u[...] = found

        @pl.when(takes)
        def _(level=level, back=back):
            back.wait_recv()
            value_v[...] = at.inbox[level][:rhs]
            value_u[...] = at.inbox[level][rhs:]

        finish.append((sends, back.wait_send))

    kept = at.kept
    found = (
        kept[order:both]
        - dot(value_v[...], embed(kept[:order]))
        - dot(value_u[...], embed(kept[both:]))
    )

    @pl.when(middle)
    def _():
        result[at_interior] = separate(reversed_where(turned, resolve(found, at.lower[...])))

    @pl.when(jnp.logical_not(middle))
    def _():
        result[at_interior] = separate(reversed_where(turned, found))

    result[1 - at_interior] = separate(value_v[...])
    for copy in sent:
        copy.wait_send()
    pl.when(shifts)(shift.wait_send)
    for condition, run in finish:
        pl.when(condition)(run)


def local(diag_blocks, couplings, sources):
    order, width = couplings.shape[1:]
    shard, rhs = diag_blocks.shape[1], sources.shape[1]
    count = order // HALF
    slabs, orbs = lax.axis_size("slab"), lax.axis_size("orb")
    levels = (slabs // 2).bit_length() - 1
    both = order + rhs
    square, tall, thin, lower = (
        (order, width), (both, width), (rhs, width), (count * (count - 1) // 2 * HALF, LANES),
    )
    dma = pltpu.SemaphoreType.DMA
    wide = (both + order, width)

    def vmem(*shape):
        return pltpu.VMEM(shape, jnp.float32)

    scratch = dict(
        diag=vmem(2, shard, width), coupling=vmem(2, order, width), load=vmem(2, rhs, width),
        interior=vmem(*square), boundary=vmem(*square), shifted=vmem(*square), pivot=vmem(*square),
        to_v=vmem(*square), outer=vmem(*square), kept=vmem(*wide), lower=vmem(*lower),
        inverse=vmem(count, LANES, LANES), across=vmem(count, LANES, (count - 1) * LANES),
        own_v=vmem(*tall), own_u=vmem(*tall), cross=vmem(*square), other=vmem(*tall),
        to_other=vmem(*square), value_v=vmem(*thin), value_u=vmem(*thin),
        fetch=dma((3,)), shift=dma((2,)), back=dma((max(1, levels), 2)),
        orb_send=dma((3, max(1, orbs - 1))), orb_receive=dma((3, max(1, orbs - 1))),
        moves=[move_semaphores(count) for _ in range(levels + 1)],
        first_v=[vmem(*tall) for _ in range(levels)],
        level_kept=[vmem(*wide) if level < levels - 1 else vmem(*tall) for level in range(levels)],
        level_lower=[vmem(*lower) for _ in range(levels)],
        outbox=[vmem(2 * rhs, width) for _ in range(levels)],
        inbox=[vmem(2 * rhs, width) for _ in range(levels)],
        first_u=[vmem(*tall) for _ in range(levels - 1)],
        first_cross=[vmem(*square) for _ in range(levels - 1)],
        extra_send=[dma((2,)) for _ in range(levels - 1)],
        extra_receive=[dma((2,)) for _ in range(levels - 1)],
    )
    leaves, tree = jax.tree.flatten(scratch)

    def held(array):
        return pltpu.with_memory_space_constraint(array, pltpu.HBM)

    return pl.pallas_call(
        functools.partial(solve_kernel, tree),
        out_shape=jax.ShapeDtypeStruct(sources.shape, jnp.float32),
        in_specs=[pl.BlockSpec(memory_space=pl.ANY)] * 3,
        out_specs=pl.BlockSpec(memory_space=pltpu.VMEM),
        scratch_shapes=leaves,
        compiler_params=pltpu.CompilerParams(
            vmem_limit_bytes=48 * 1024 * 1024, collective_id=0, has_side_effects=True
        ),
    )(held(diag_blocks), held(couplings), held(sources))


def solution(mesh):
    placed = (
        P(("energy", "slab"), "orb", None),
        P(("energy", "slab"), None, None),
        P(("energy", "slab"), ("orb", "rhs"), None),
    )
    return jax.shard_map(
        local,
        mesh=mesh,
        in_specs=placed,
        out_specs=P(("energy", "slab"), ("orb", "rhs"), None),
        check_vma=False,
    )
```
